32 devices in a mesh: row: 2 (over y), col: 16 (over z, x, core).
Axes of the slice: x: 2, y: 2, z: 4, core: 2. Of those that a mesh axis runs over, the one named last changes fastest.
Arguments:
- tokens: bfloat16 [512, 1024], P(('row', 'col')), may hold values from -6 to 6
- grad_out: bfloat16 [512, 1024], P(('row', 'col')), may hold values from -1.1953125 to 1.1953125
- gains: float32 [2, 1024], replicated, may hold values from 0.1 to 1.9
- flat_in: bfloat16 [16384, 2048], P(('row', 'col')), may hold values from -0.1875 to 0.1875
- flat_out: bfloat16 [16384, 2048], P(('row', 'col')), may hold values from -0.03125 to 0.03125
- flat_moment: float32 [2, 16384, 2048], P(None, ('row', 'col')), may hold values from -3 to 3
- flat_second: float32 [2, 16384, 2048], P(None, ('row', 'col')), may hold values from 0.05 to 2
- tile_in: bfloat16 [16, 6, 256, 2048], P('col', 'row'), may hold values from -0.1875 to 0.1875
- tile_out: bfloat16 [16, 6, 256, 2048], P('col', 'row'), may hold values from -0.03125 to 0.03125
- tile_moment: float32 [2, 16, 6, 256, 2048], P(None, 'col', 'row'), may hold values from -3 to 3
- tile_second: float32 [2, 16, 6, 256, 2048], P(None, 'col', 'row'), may hold values from 0.05 to 2
- owners: int32 [2, 16, 4], P(None, 'col'), may hold values from 0 to 1, as said below
Outputs:
- hidden_out: bfloat16 [512, 1024], P(('row', 'col'))
- grad_tokens: bfloat16 [512, 1024], P(('row', 'col'))
- new_flat_in: bfloat16 [16384, 2048], P(('row', 'col'))
- new_flat_out: bfloat16 [16384, 2048], P(('row', 'col'))
- new_flat_moment: float32 [2, 16384, 2048], P(None, ('row', 'col'))
- new_flat_second: float32 [2, 16384, 2048], P(None, ('row', 'col'))
- new_tile_in: bfloat16 [16, 6, 256, 2048], P('col', 'row')
- new_tile_out: bfloat16 [16, 6, 256, 2048], P('col', 'row')
- new_tile_moment: float32 [2, 16, 6, 256, 2048], P(None, 'col', 'row')
- new_tile_second: float32 [2, 16, 6, 256, 2048], P(None, 'col', 'row')
The draws below stay inside these ranges and needn't reach their ends.
Inputs may be any that keep to these rules, and one draw needn't show every extreme that they name: `owners`: for each matrix and column block, entry k names the row that owns tile k; each row owns at most 3 tiles of a block and matrix, and in each block and matrix some row owns exactly 3.
All inputs are finite; a program needn't handle non-finite values.
Results may differ from the reference program's by a relative error of at most 0.029.
Values may be sent and summed in bfloat16 or wider, within the bound.
A program may use at most 192 MiB of HBM per device.

```python
import math
import jax
import jax.numpy as jnp
from jax import lax

D = 1024
FF = 32768
OWN_CAP = 3
TOKENS = 512
GROUP_TOK = 256
BLOCK = 2048
TILES = 4
TILE_ROWS = 256
N_ROW = 2
N_COL = 16


def draw_owners(key, part):
    owner_pool = jnp.repeat(jnp.arange(N_ROW, dtype=jnp.int32), OWN_CAP)

    def one_block(sub_key):
        key_full, key_pick, key_order = jax.random.split(sub_key, 3)
        favored = jax.random.randint(key_full, (), 0, N_ROW, dtype=jnp.int32)
        scores = jax.random.permutation(key_pick, N_ROW * OWN_CAP).astype(jnp.int32) + jnp.where(owner_pool == favored, N_ROW * OWN_CAP, 0).astype(jnp.int32)
        picked = jnp.argsort(-scores, stable=True)[:2 * N_ROW]
        chosen = owner_pool[picked]
        return chosen[jax.random.permutation(key_order, 2 * N_ROW)]
    block_keys = jax.random.split(jax.random.fold_in(key, 17), 2 * N_COL)
    return jax.vmap(one_block)(block_keys).reshape(2, N_COL, 2 * N_ROW).astype(jnp.int32)


def block_levels(own_key, dims, cuts, least, high):
    factor_of, own = 1.0, jax.random.fold_in(own_key, 6)
    for position, shards_of in cuts:
        draws = jnp.exp(jax.random.uniform(jax.random.fold_in(own, position), (shards_of,), jnp.float32, least / len(cuts), high / len(cuts)))
        factor_of = factor_of * jnp.repeat(draws, dims[position] // shards_of).reshape([-1 if axis == position else 1 for axis in range(len(dims))])
    return factor_of


def bell_draw(rng, dims, deviation, reach, cuts=(), kind=jnp.bfloat16):
    drawn = jax.random.normal(rng, dims, jnp.float32) * deviation
    if len(cuts) > 0:
        drawn = block_levels(rng, dims, cuts, -0.22, 0.18) * drawn
    return jnp.clip(drawn, min=-reach, max=reach).astype(kind)


def setup_inputs(seed: int = 0) -> dict:
    streams_of = jax.random.split(jax.random.key(seed), 13)
    tokens = bell_draw(streams_of[0], (TOKENS, D), 1.0, 6.0, ((0, 32),))
    grad_out = bell_draw(streams_of[1], (TOKENS, D), 0.2, 1.1953125, ((0, 32),))
    gains = jnp.clip(1.0 + 0.18 * jax.random.normal(streams_of[2], (2, D), jnp.float32), 0.1, 1.9)
    flat_in = bell_draw(streams_of[3], (D * N_COL, BLOCK), D ** -0.5, 0.1875, ((0, 32),))
    flat_out = bell_draw(streams_of[4], (D * N_COL, BLOCK), FF ** -0.5, 0.03125, ((0, 32),))
    flat_moment = bell_draw(streams_of[5], (2, D * N_COL, BLOCK), 0.5, 3.0, ((1, 32),), jnp.float32)
    flat_second = jnp.clip(jnp.exp(math.log(2.0) - 3.6888794 * jax.random.uniform(streams_of[6], (2, D * N_COL, BLOCK), jnp.float32) ** block_levels(streams_of[6], (2, D * N_COL, BLOCK), ((1, 32),), -0.2, 0.2)), 0.05, 2.0)
    tile_in = bell_draw(streams_of[7], (N_COL, N_ROW * OWN_CAP, TILE_ROWS, BLOCK), D ** -0.5, 0.1875, ((0, 16), (1, 2)))
    tile_out = bell_draw(streams_of[8], (N_COL, N_ROW * OWN_CAP, TILE_ROWS, BLOCK), FF ** -0.5, 0.03125, ((0, 16), (1, 2)))
    tile_moment = bell_draw(streams_of[9], (2, N_COL, N_ROW * OWN_CAP, TILE_ROWS, BLOCK), 0.5, 3.0, ((1, 16), (2, 2)), jnp.float32)
    tile_second = jnp.clip(jnp.exp(math.log(2.0) - 3.6888794 * jax.random.uniform(streams_of[10], (2, N_COL, N_ROW * OWN_CAP, TILE_ROWS, BLOCK), jnp.float32) ** block_levels(streams_of[10], (2, N_COL, N_ROW * OWN_CAP, TILE_ROWS, BLOCK), ((1, 16), (2, 2)), -0.2, 0.2)), 0.05, 2.0)
    owners = draw_owners(jax.random.fold_in(streams_of[12], 71), 0)
    return dict(tokens=tokens, grad_out=grad_out, gains=gains, flat_in=flat_in, flat_out=flat_out, flat_moment=flat_moment, flat_second=flat_second, tile_in=tile_in, tile_out=tile_out, tile_moment=tile_moment, tile_second=tile_second, owners=owners)


norm_eps = 1e-06
beta_one = 0.9
beta_two = 0.95
learn_rate = 0.002
decay_rate = 0.1
adam_eps = 1e-08
gelu_coef = 0.7978845608

def gelu_value(hidden):
    tanh_term = jnp.tanh(gelu_coef * (hidden + 0.044715 * hidden * hidden * hidden))
    return 0.5 * hidden * (1.0 + tanh_term)

def gelu_slope(hidden):
    tanh_term = jnp.tanh(gelu_coef * (hidden + 0.044715 * hidden * hidden * hidden))
    return 0.5 * (1.0 + tanh_term) + 0.5 * hidden * (1.0 - tanh_term * tanh_term) * gelu_coef * (1.0 + 0.134145 * hidden * hidden)

def adam_update(weight, gradient, moment, second):
    new_moment = beta_one * moment + (1.0 - beta_one) * gradient
    new_second = beta_two * second + (1.0 - beta_two) * gradient * gradient
    weight_float = weight.astype(jnp.float32)
    stepped = weight_float - learn_rate * (new_moment / (jnp.sqrt(new_second) + adam_eps) + decay_rate * weight_float)
    return (stepped.astype(jnp.bfloat16), new_moment, new_second)

def slot_tables(owner_rows, slot_cap, row_total):
    tile_count = owner_rows.shape[-1]
    positions = jnp.arange(tile_count, dtype=jnp.int32)
    same_owner = owner_rows[..., :, None] == owner_rows[..., None, :]
    earlier = positions[None, :] < positions[:, None]
    tile_rank = lax.optimization_barrier(jnp.sum(jnp.where(same_owner & earlier, 1, 0), axis=-1)).astype(jnp.int32)
    slot_dest = (owner_rows * slot_cap + tile_rank).astype(jnp.int32)
    slot_ids = jnp.arange(row_total * slot_cap, dtype=jnp.int32)
    matches = slot_dest[..., None, :] == slot_ids[:, None]
    slot_tile = lax.optimization_barrier(jnp.sum(jnp.where(matches, positions, 0), axis=-1)).astype(jnp.int32)
    slot_live = jnp.any(matches, axis=-1)
    return (slot_dest, slot_tile, slot_live)

def layer_forward(layer_in, gain_vec, w_in, w_out):
    tok_float = layer_in.astype(jnp.float32)
    inv_rms = lax.rsqrt(lax.optimization_barrier(jnp.mean(tok_float * tok_float, axis=1, keepdims=True)) + norm_eps)
    normed = (tok_float * inv_rms * gain_vec).astype(jnp.bfloat16)
    hidden = jnp.dot(normed, w_in, preferred_element_type=jnp.float32)
    activated = gelu_value(hidden).astype(jnp.bfloat16)
    mixed_sum = lax.dot_general(activated, w_out, (((1,), (1,)), ((), ())), preferred_element_type=jnp.float32)
    return ((tok_float + mixed_sum).astype(jnp.bfloat16), (tok_float, inv_rms, normed, hidden, activated))

def group_sums(left_rows, right_rows):
    left_groups = left_rows.reshape(N_ROW, GROUP_TOK, left_rows.shape[1])
    right_groups = right_rows.reshape(N_ROW, GROUP_TOK, right_rows.shape[1])

    def add_group(running, operands):
        product = lax.dot_general(operands[0], operands[1], (((0,), (0,)), ((), ())), preferred_element_type=jnp.float32)
        rounded = lax.optimization_barrier(product.astype(jnp.bfloat16))
        return (running + rounded.astype(jnp.float32), None)
    start_sum = jnp.zeros((left_rows.shape[1], right_rows.shape[1]), jnp.float32)
    running, unused = lax.scan(add_group, start_sum, (left_groups, right_groups))
    return running

def layer_backward(cotangent, gain_vec, w_in, w_out, saved_state):
    tok_float, inv_rms, normed, hidden, activated = saved_state
    d_act = jnp.dot(cotangent, w_out, preferred_element_type=jnp.float32)
    d_hidden = (d_act * gelu_slope(hidden)).astype(jnp.bfloat16)
    d_normed = lax.dot_general(d_hidden, w_in, (((1,), (1,)), ((), ())), preferred_element_type=jnp.float32)
    gated = d_normed * gain_vec
    tok_grad = cotangent.astype(jnp.float32) + inv_rms * gated - tok_float * inv_rms * inv_rms * inv_rms * lax.optimization_barrier(jnp.mean(tok_float * gated, axis=1, keepdims=True))
    grad_in = group_sums(normed, d_hidden)
    grad_wout = group_sums(cotangent, activated)
    return (tok_grad.astype(jnp.bfloat16), grad_in, grad_wout)

def assemble(slot_data, slot_dest_m):
    tile_data = jnp.take_along_axis(slot_data, slot_dest_m[:, :, None, None], axis=1)
    return tile_data.transpose(1, 2, 0, 3).reshape(D, FF)

def tiled_update(slot_data, gradient, moment, second, slot_tile_m, slot_live_m):
    grad_tiles = gradient.reshape(TILES, TILE_ROWS, N_COL, BLOCK).transpose(2, 0, 1, 3)
    grad_slots = jnp.take_along_axis(grad_tiles, slot_tile_m[:, :, None, None], axis=1)
    new_weight, new_moment, new_second = adam_update(slot_data, grad_slots, moment, second)
    live_mask = slot_live_m[:, :, None, None]
    return (jnp.where(live_mask, new_weight, slot_data), jnp.where(live_mask, new_moment, moment), jnp.where(live_mask, new_second, second))

def reference(tokens, grad_out, gains, flat_in, flat_out, flat_moment, flat_second, tile_in, tile_out, tile_moment, tile_second, owners):
    slot_dest, slot_tile, slot_live = slot_tables(owners, OWN_CAP, N_ROW)
    first_in = flat_in.reshape(D, FF)
    first_out = flat_out.reshape(D, FF)
    second_in = assemble(tile_in, slot_dest[0])
    second_out = assemble(tile_out, slot_dest[1])
    middle, saved_one = layer_forward(tokens, gains[0], first_in, first_out)
    hidden_out, saved_two = layer_forward(middle, gains[1], second_in, second_out)
    grad_mid, grad_in_two, grad_out_two = layer_backward(grad_out, gains[1], second_in, second_out, saved_two)
    grad_tokens, grad_in_one, grad_out_one = layer_backward(grad_mid, gains[0], first_in, first_out, saved_one)
    new_flat_in, moment_in, second_in_f = adam_update(flat_in, grad_in_one.reshape(D * N_COL, BLOCK), flat_moment[0], flat_second[0])
    new_flat_out, moment_out, second_out_f = adam_update(flat_out, grad_out_one.reshape(D * N_COL, BLOCK), flat_moment[1], flat_second[1])
    new_tile_in, tmoment_in, tsecond_in = tiled_update(tile_in, grad_in_two, tile_moment[0], tile_second[0], slot_tile[0], slot_live[0])
    new_tile_out, tmoment_out, tsecond_out = tiled_update(tile_out, grad_out_two, tile_moment[1], tile_second[1], slot_tile[1], slot_live[1])
    return (hidden_out, grad_tokens, new_flat_in, new_flat_out, jnp.stack([moment_in, moment_out]), jnp.stack([second_in_f, second_out_f]), new_tile_in, new_tile_out, jnp.stack([tmoment_in, tmoment_out]), jnp.stack([tsecond_in, tsecond_out]))
```

```python
import functools

import jax
import jax.numpy as jnp
from jax import lax
from jax.experimental import pallas as pl
from jax.experimental.pallas import tpu as pltpu
from jax.sharding import PartitionSpec as P

norm_eps = 1e-06
beta_one = 0.9
beta_two = 0.95
learn_rate = 0.002
decay_rate = 0.1
adam_eps = 1e-08
gelu_coef = 0.7978845608
both = ("row", "col")


def gelu_both(hidden):
    square = hidden * hidden
    tanh_term = jnp.tanh(gelu_coef * (hidden + 0.044715 * square * hidden))
    value = 0.5 * hidden * (1.0 + tanh_term)
    slope = 0.5 * (1.0 + tanh_term) + 0.5 * hidden * (1.0 - tanh_term * tanh_term) * gelu_coef * (
        1.0 + 0.134145 * square
    )
    return value, slope


def adam_update(weight, gradient, moment, second):
    new_moment = beta_one * moment + (1.0 - beta_one) * gradient
    new_second = beta_two * second + (1.0 - beta_two) * gradient * gradient
    weight_float = weight.astype(jnp.float32)
    stepped = weight_float - learn_rate * (
        new_moment / (jnp.sqrt(new_second) + adam_eps) + decay_rate * weight_float
    )
    return (stepped.astype(jnp.bfloat16), new_moment, new_second)


def tile_ranks(owner_rows):
    positions = jnp.arange(owner_rows.shape[-1], dtype=jnp.int32)
    same_owner = owner_rows[..., :, None] == owner_rows[..., None, :]
    earlier = positions[None, :] < positions[:, None]
    return jnp.sum(jnp.where(same_owner & earlier, 1, 0), axis=-1).astype(jnp.int32)


def flat_kernel(w_in, w_out, g_in, g_out, mom, sec, o_in, o_out, o_mom, o_sec):
    for m, (w, g, o) in enumerate(((w_in, g_in, o_in), (w_out, g_out, o_out))):
        new = adam_update(w[...], g[...].astype(jnp.float32), mom[m], sec[m])
        o[...], o_mom[m], o_sec[m] = new


def flat_adam(w_in, w_out, g_in, g_out, mom, sec):
    rows, width = w_in.shape
    step = min(rows, 32)
    thin = pl.BlockSpec((step, width), lambda i: (i, 0))
    wide = pl.BlockSpec((2, step, width), lambda i: (0, i, 0))
    shape = jax.ShapeDtypeStruct
    return pl.pallas_call(
        flat_kernel,
        grid=(rows // step,),
        in_specs=[thin, thin, thin, thin, wide, wide],
        out_specs=[thin, thin, wide, wide],
        out_shape=[
            shape(w_in.shape, w_in.dtype),
            shape(w_out.shape, w_out.dtype),
            shape(mom.shape, mom.dtype),
            shape(sec.shape, sec.dtype),
        ],
        cost_estimate=pl.CostEstimate(
            flops=30 * mom.size, bytes_accessed=20 * mom.size + 2 * mom.size, transcendentals=mom.size
        ),
        name="flat_adam",
    )(w_in, w_out, g_in, g_out, mom, sec)


def tile_kernel(
    tiles, live, me, l_in, l_out, r_in, r_out, w_in, w_out, mom, sec, o_in, o_out, o_mom, o_sec
):
    slot = pl.program_id(0)
    parts = ((l_in, r_in, w_in, o_in), (l_out, r_out, w_out, o_out))
    for m, (left, right, w, o) in enumerate(parts):
        grad = jnp.dot(left[...], right[0], preferred_element_type=jnp.float32)
        alive = live[m, slot] > 0
        old_w, old_m, old_s = w[0, 0], mom[m, 0, 0], sec[m, 0, 0]
        new_w, new_m, new_s = adam_update(old_w, grad, old_m, old_s)
        o[0, 0] = jnp.where(alive, new_w.astype(jnp.float32), old_w.astype(jnp.float32)).astype(
            jnp.bfloat16
        )
        o_mom[m, 0, 0] = jnp.where(alive, new_m, old_m)
        o_sec[m, 0, 0] = jnp.where(alive, new_s, old_s)


def tile_adam(tiles, live, me, l_in, l_out, r_in, r_out, w_in, w_out, mom, sec):
    slot_cap, tile_rows, width = w_in.shape[1:]
    ranks, toks, sub = r_in.shape
    step = min(sub, 512)
    per = sub // step

    def left_map(m):
        return lambda s, h, tiles, live, me: (tiles[m, s], 0)

    def right_map(s, h, tiles, live, me):
        return (lax.rem(me[0] + ranks - h // per, ranks), 0, h % per)

    def thin_map(s, h, *unused):
        return (0, s, 0, h)

    def wide_map(s, h, *unused):
        return (0, 0, s, 0, h)

    right = pl.BlockSpec((1, toks, step), right_map)
    thin = pl.BlockSpec((1, 1, tile_rows, step), thin_map)
    wide = pl.BlockSpec((2, 1, 1, tile_rows, step), wide_map)
    shape = jax.ShapeDtypeStruct
    return pl.pallas_call(
        tile_kernel,
        grid_spec=pltpu.PrefetchScalarGridSpec(
            num_scalar_prefetch=3,
            grid=(slot_cap, width // step),
            in_specs=[
                pl.BlockSpec((tile_rows, toks), left_map(0)),
                pl.BlockSpec((tile_rows, toks), left_map(1)),
                right,
                right,
                thin,
                thin,
                wide,
                wide,
            ],
            out_specs=[thin, thin, wide, wide],
        ),
        out_shape=[
            shape(w_in.shape, w_in.dtype),
            shape(w_out.shape, w_out.dtype),
            shape(mom.shape, mom.dtype),
            shape(sec.shape, sec.dtype),
        ],
        cost_estimate=pl.CostEstimate(
            flops=2 * toks * mom.size, bytes_accessed=22 * mom.size, transcendentals=mom.size
        ),
        name="tile_adam",
    )(tiles, live, me, l_in, l_out, r_in, r_out, w_in, w_out, mom, sec)


def row_swap(pieces_for, row_total):
    got = [pieces_for(0)]
    for shift in range(1, row_total):
        pairs = [(src, (src + shift) % row_total) for src in range(row_total)]
        got.append(lax.ppermute(pieces_for(shift), "row", pairs))
    return jnp.stack(got)


def spread_sum(partial, total):
    toks, width = partial.shape
    sent = partial.astype(jnp.bfloat16)
    came = lax.all_to_all(sent, both, split_axis=0, concat_axis=0, tiled=True)
    return jnp.sum(came.reshape(total, toks // total, width).astype(jnp.float32), axis=0)


def late_sum(partial):
    return lax.psum_scatter(
        partial.astype(jnp.bfloat16), both, scatter_dimension=0, tiled=True
    ).astype(jnp.float32)


def dot_nt(left, right):
    return lax.dot_general(left, right, (((1,), (1,)), ((), ())), preferred_element_type=jnp.float32)


def dot_tn(left, right):
    return lax.dot_general(left, right, (((0,), (0,)), ((), ())), preferred_element_type=jnp.float32)


def norm_of(layer_in, gain_vec):
    tok_float = layer_in.astype(jnp.float32)
    inv_rms = lax.rsqrt(jnp.mean(tok_float * tok_float, axis=1, keepdims=True) + norm_eps)
    normed = (tok_float * inv_rms * gain_vec).astype(jnp.bfloat16)
    return tok_float, inv_rms, normed


def token_grad(cotangent, d_normed, gain_vec, tok_float, inv_rms):
    gated = d_normed * gain_vec
    return (
        cotangent.astype(jnp.float32)
        + inv_rms * gated
        - tok_float
        * inv_rms
        * inv_rms
        * inv_rms
        * jnp.mean(tok_float * gated, axis=1, keepdims=True)
    ).astype(jnp.bfloat16)


def shards(
    tokens,
    grad_out,
    gains,
    flat_in,
    flat_out,
    flat_moment,
    flat_second,
    tile_in,
    tile_out,
    tile_moment,
    tile_second,
    owners,
):
    row_total = lax.axis_size("row")
    col_total = lax.axis_size("col")
    dims = fused_dims(row_total, col_total, tokens, flat_in, tile_in, owners)
    if dims is not None:
        return fused_shards(
            dims,
            tokens,
            grad_out,
            gains,
            flat_in,
            flat_out,
            flat_moment,
            flat_second,
            tile_in,
            tile_out,
            tile_moment,
            tile_second,
            owners,
        )
    total = row_total * col_total
    row_index = lax.axis_index("row")
    model_width = tokens.shape[1]
    block = flat_in.shape[1]
    sub = block // row_total
    own_rows = flat_in.shape[0] // col_total
    slot_cap = tile_in.shape[1]
    tile_rows = tile_in.shape[2]

    owner_rows = owners[:, 0, :]
    ranks = tile_ranks(owner_rows)
    came_from = lax.rem(row_index - owner_rows + row_total, row_total)
    slot_pick = came_from * slot_cap + ranks
    slots = jnp.arange(slot_cap, dtype=jnp.int32)[None, :, None]
    mine = (owner_rows == row_index)[:, None, :] & (ranks[:, None, :] == slots)
    positions = jnp.arange(owner_rows.shape[1], dtype=jnp.int32)
    my_tiles = jnp.sum(jnp.where(mine, positions, 0), axis=-1).astype(jnp.int32)
    my_live = jnp.any(mine, axis=-1).astype(jnp.int32)

    def flat_to_units(flat):
        parts = flat.reshape(own_rows, col_total, row_total, sub).transpose(2, 1, 0, 3)
        return lax.all_to_all(
            parts.reshape(total * own_rows, sub), both, split_axis=0, concat_axis=0, tiled=True
        )

    def units_to_flat(grad):
        came = lax.all_to_all(
            grad.astype(jnp.bfloat16), both, split_axis=0, concat_axis=0, tiled=True
        )
        parts = came.reshape(row_total, col_total, own_rows, sub).transpose(2, 1, 0, 3)
        return parts.reshape(own_rows * col_total, block)

    def tiles_to_units(tile, pick):
        def piece(shift):
            to_row = lax.rem(row_index + shift, row_total)
            return lax.dynamic_slice_in_dim(tile[0], to_row * sub, sub, 2)

        whole = row_swap(piece, row_total).reshape(row_total * slot_cap, tile_rows, sub)
        return jnp.take(whole, pick, axis=0).reshape(model_width, sub)

    def gather(x):
        return lax.all_gather(x, both, axis=0, tiled=True)

    tok_one, inv_one, normed_one = norm_of(tokens, gains[0])
    normed_one = gather(normed_one)
    one_in = flat_to_units(flat_in)
    one_out = flat_to_units(flat_out)
    cot_two = gather(grad_out)
    two_in = tiles_to_units(tile_in, slot_pick[0])
    two_out = tiles_to_units(tile_out, slot_pick[1])
    hidden_one = jnp.dot(normed_one, one_in, preferred_element_type=jnp.float32)
    act_one, slope_one = gelu_both(hidden_one)
    act_one = act_one.astype(jnp.bfloat16)
    middle = (tok_one + spread_sum(dot_nt(act_one, one_out), total)).astype(jnp.bfloat16)

    tok_two, inv_two, normed_two = norm_of(middle, gains[1])
    normed_two = gather(normed_two)
    hidden_two = jnp.dot(normed_two, two_in, preferred_element_type=jnp.float32)
    act_two, slope_two = gelu_both(hidden_two)
    act_two = act_two.astype(jnp.bfloat16)
    d_act_two = jnp.dot(cot_two, two_out, preferred_element_type=jnp.float32)
    d_hidden_two = (d_act_two * slope_two).astype(jnp.bfloat16)
    d_normed_two = spread_sum(dot_nt(d_hidden_two, two_in), total)
    grad_mid = token_grad(grad_out, d_normed_two, gains[1], tok_two, inv_two)
    cot_one = gather(grad_mid)

    d_act_one = jnp.dot(cot_one, one_out, preferred_element_type=jnp.float32)
    d_hidden_one = (d_act_one * slope_one).astype(jnp.bfloat16)
    flat_grad_in = units_to_flat(dot_tn(normed_one, d_hidden_one))
    flat_grad_out = units_to_flat(dot_tn(cot_one, act_one))

    act_late, _ = lax.optimization_barrier((act_two, cot_one))
    mixed_two = late_sum(dot_nt(act_late, two_out))
    hidden_out = (tok_two + mixed_two).astype(jnp.bfloat16)
    d_normed_one = late_sum(dot_nt(d_hidden_one, one_in))
    grad_tokens = token_grad(grad_mid, d_normed_one, gains[0], tok_one, inv_one)

    d_hidden_rows = row_swap(lambda shift: d_hidden_two, row_total)
    act_rows = row_swap(lambda shift: act_two, row_total)
    new_tile = tile_adam(
        my_tiles,
        my_live,
        row_index.astype(jnp.int32).reshape(1),
        normed_two.T,
        cot_two.T,
        d_hidden_rows,
        act_rows,
        tile_in,
        tile_out,
        tile_moment,
        tile_second,
    )
    new_flat = flat_adam(flat_in, flat_out, flat_grad_in, flat_grad_out, flat_moment, flat_second)
    return (hidden_out, grad_tokens, *new_flat, *new_tile)


MESH = pl.DeviceIdType.MESH


def middle_kernel(
    dims,
    pick,
    tok_ref,
    gout_ref,
    gains_ref,
    flat_in,
    flat_out,
    tile_in,
    tile_out,
    hid_out,
    gtok_out,
    gr_out,
    act_out,
    dh_out,
    n2_out,
    c2_out,
    stage,
    send,
    weights,
    slots_in,
    slots_out,
    g1,
    gc,
    g2,
    gm,
    act1,
    slope1,
    dact2,
    act2,
    dh2,
    dh1,
    grads,
    psend,
    pown,
    rcore,
    s1,
    rxy,
    s2,
    rz,
    mid_ref,
    gmid_ref,
    stage_sem,
    a2a_send,
    a2a_recv,
    slot_local,
    slot_send,
    slot_recv,
    ag_send,
    ag_recv,
    rs_send,
    rs_recv,
    out_sem,
):
    rows, zs, xs, tok, width, units, per, slot_cap, tiles = dims
    cols = zs * xs * 2
    total = rows * cols
    groups = rows * zs * xs
    all_tok = total * tok
    step = 256
    unit_steps = units // step
    width_steps = width // step
    r = lax.axis_index("row")
    c = lax.axis_index("col")
    me = r * cols + c
    core = lax.rem(c, 2)
    x = lax.rem(c // 2, xs)
    z = c // (2 * xs)
    f32, bf16 = jnp.float32, jnp.bfloat16

    def col_of(zi, xi, ci):
        return (zi * xs + xi) * 2 + ci

    def remote(src, dst, ssem, rsem, row_to, col_to):
        return pltpu.make_async_remote_copy(
            src_ref=src,
            dst_ref=dst,
            send_sem=ssem,
            recv_sem=rsem,
            device_id=(row_to, col_to),
            device_id_type=MESH,
        )

    plane = [(dr, dx) for dr in range(rows) for dx in range(xs) if (dr, dx) != (0, 0)]

    def ag_z(g, n):
        out = []
        for dz in range(1, zs):
            zt = lax.rem(z + dz, zs)
            here = g.at[r, z, x, core]
            out.append(
                remote(here, here, ag_send.at[n, dz], ag_recv.at[n, dz], r, col_of(zt, x, core))
            )
        for cp in out:
            cp.start()
        return out

    def ag_xy(g, n):
        out = []
        for j, (dr, dx) in enumerate(plane):
            rt, xt = lax.rem(r + dr, rows), lax.rem(x + dx, xs)
            here = g.at[r, :, x, core]
            out.append(
                remote(
                    here,
                    here,
                    ag_send.at[n, zs + j],
                    ag_recv.at[n, zs + j],
                    rt,
                    col_of(z, xt, core),
                )
            )
        for cp in out:
            cp.start()
        return out

    def ag_core(g, n):
        here = g.at[:, :, :, core]
        cp = remote(here, here, ag_send.at[n, 0], ag_recv.at[n, 0], r, col_of(z, x, 1 - core))
        cp.start()
        return [cp]

    def arrived(copies):
        for cp in copies:
            cp.wait_recv()

    def flat_of(g, lo, size):
        return g[:, :, :, :, :, lo : lo + size].reshape(all_tok, size)

    def dot(a, b):
        return jnp.dot(a, b, preferred_element_type=f32)

    def rs_core(n, lhs, rhs):
        def half(which, store):
            left = lhs[:, pl.ds(which, 1)].reshape(groups * tok, units)

            def tile(j, carry):
                at = pl.ds(pl.multiple_of(j * step, step), step)
                store(at, dot_nt(left, rhs(j)).reshape(groups, tok, step))
                return carry

            lax.fori_loop(0, width_steps, tile, 0)

        def to_send(at, value):
            psend[n, :, :, at] = value.astype(bf16)

        def to_own(at, value):
            pown[n, :, :, at] = value

        half(1 - core, to_send)
        cp = remote(
            psend.at[n], rcore.at[n], rs_send.at[n, 0], rs_recv.at[n, 0], r, col_of(z, x, 1 - core)
        )
        cp.start()
        half(core, to_own)
        return [cp]

    def rs_xy(n):
        def add(k, carry):
            value = pown[n, k] + rcore[n, k].astype(f32)
            s1[n, k // (zs * xs), lax.rem(k // xs, zs), lax.rem(k, xs)] = value.astype(bf16)
            return carry

        lax.fori_loop(0, groups, add, 0)
        out = []
        for j, (dr, dx) in enumerate(plane):
            rt, xt = lax.rem(r + dr, rows), lax.rem(x + dx, xs)
            out.append(
                remote(
                    s1.at[n, rt, :, xt],
                    rxy.at[n, j],
                    rs_send.at[n, 1 + j],
                    rs_recv.at[n, 1 + j],
                    rt,
                    col_of(z, xt, core),
                )
            )
        for cp in out:
            cp.start()
        return out

    def rs_z(n):
        def add(k, carry):
            value = s1[n, r, k, x].astype(f32)
            for j in range(len(plane)):
                value = value + rxy[n, j, k].astype(f32)
            s2[n, k] = value.astype(bf16)
            return carry

        lax.fori_loop(0, zs, add, 0)
        out = []
        for dz in range(1, zs):
            zt = lax.rem(z + dz, zs)
            j = len(plane) + dz
            out.append(
                remote(
                    s2.at[n, zt],
                    rz.at[n, dz],
                    rs_send.at[n, j],
                    rs_recv.at[n, j],
                    r,
                    col_of(zt, x, core),
                )
            )
        for cp in out:
            cp.start()
        return out

    def rs_end(n):
        value = s2[n, z].astype(f32)
        for dz in range(1, zs):
            value = value + rz[n, dz].astype(f32)
        return value

    def a2a_start(m, first):
        def one(k, carry):
            to = lax.rem(me + k, total)
            rt, ct = to // cols, lax.rem(to, cols)
            at = pl.ds(pl.multiple_of(me * per, per), per)
            remote(send.at[m, rt, ct], weights.at[m, at], a2a_send.at[m], a2a_recv.at[m], rt, ct).start()
            return carry

        lax.fori_loop(first, total, one, 0)

    def a2a_part(m):
        span = weights.at[m, pl.ds(0, (total - 1) * per)]
        return remote(span, span, a2a_send.at[m], a2a_recv.at[m], r, c)

    def permute(m):
        rows_in = cols * 16
        p = lax.broadcasted_iota(jnp.int32, (rows_in, rows_in), 0)
        q = lax.broadcasted_iota(jnp.int32, (rows_in, rows_in), 1)
        swap = (lax.rem(p, 16) == q // cols) & (p // 16 == lax.rem(q, cols))
        swap = jnp.where(swap, 1.0, 0.0).astype(bf16)

        def block(k, carry):
            b, h = k // unit_steps, lax.rem(k, unit_steps)
            from_rows = pl.ds(pl.multiple_of(b * rows_in, rows_in), rows_in)
            for rt in range(rows):
                lanes = pl.ds(pl.multiple_of(rt * units + h * step, step), step)
                got = dot(swap, stage[m, from_rows, lanes]).astype(bf16).reshape(cols, 16, step)
                to_rows = pl.ds(pl.multiple_of(b * 16, 16), 16)
                to_lanes = pl.ds(pl.multiple_of(h * step, step), step)
                send[m, rt, :, to_rows, to_lanes] = got
            return carry

        lax.fori_loop(0, (per // 16) * unit_steps, block, 0)
        weights[m, pl.ds(pl.multiple_of(me * per, per), per), :] = send[m, r, c]

    loads = [
        pltpu.make_async_copy(flat, stage.at[m], stage_sem.at[m])
        for m, flat in enumerate((flat_in, flat_out))
    ]
    for cp in loads:
        cp.start()

    x_one = tok_ref[...].astype(f32)
    inv_one = lax.rsqrt(jnp.mean(x_one * x_one, axis=1, keepdims=True) + norm_eps)
    gain_one = gains_ref[0:1, :]
    gain_two = gains_ref[1:2, :]
    g1[r, z, x, core] = (x_one * inv_one * gain_one).astype(bf16)
    gc[r, z, x, core] = gout_ref[...]
    sent = []
    one_z = ag_z(g1, 0)
    cot_z = ag_z(gc, 1)

    loads[0].wait()
    permute(0)
    arrived(one_z)
    arrived(cot_z)
    one_xy = ag_xy(g1, 0)
    cot_xy = ag_xy(gc, 1)
    a2a_start(0, 1)
    loads[1].wait()
    permute(1)
    arrived(one_xy)
    arrived(cot_xy)
    one_c = ag_core(g1, 0)
    cot_c = ag_core(gc, 1)
    a2a_start(1, 1)

    tile_refs = (tile_in, tile_out)
    slots = (slots_in, slots_out)
    slot_copies = []
    for m in (1, 0):
        for dr in range(rows):
            rt = lax.rem(r + dr, rows)
            src = tile_refs[m].at[0, :, :, pl.ds(pl.multiple_of(rt * units, units), units)]
            if dr == 0:
                cp = pltpu.make_async_copy(src, slots[m].at[r], slot_local.at[m])
            else:
                cp = remote(
                    src, slots[m].at[r], slot_send.at[m, dr], slot_recv.at[m, dr], rt, c
                )
            cp.start()
            slot_copies.append((m, dr, cp))

    def slots_arrived(m):
        for mm, dr, cp in slot_copies:
            if mm == m:
                if dr == 0:
                    cp.wait()
                else:
                    cp.wait_recv()

    arrived(one_c)
    arrived(cot_c)
    outs = []
    for j, (src, dst) in enumerate(((gc, c2_out),)):
        cp = pltpu.make_async_copy(src, dst, out_sem.at[0])
        cp.start()
        outs.append(cp)

    a2a_part(0).wait_recv()

    def hidden_one(j, carry):
        at = pl.ds(pl.multiple_of(j * step, step), step)
        act, slope = gelu_both(dot(flat_of(g1, 0, width), weights[0, :, at]))
        act1[:, :, :, at] = act.astype(bf16).reshape(groups, 2, tok, step)
        slope1[:, at] = slope
        return carry

    lax.fori_loop(0, unit_steps, hidden_one, 0)
    a2a_part(1).wait_recv()

    def out_rows(j):
        return weights[1, pl.ds(pl.multiple_of(j * step, step), step), :]

    def in_rows(j):
        return weights[0, pl.ds(pl.multiple_of(j * step, step), step), :]

    mix_c = rs_core(0, act1, out_rows)
    arrived(mix_c)
    mix_xy = rs_xy(0)

    slots_arrived(1)

    def cot_act(j, carry):
        at = pl.ds(pl.multiple_of(j * step, step), step)
        value = None
        for k in range(tiles):
            where = pick[tiles + k]
            rhs = slots_out[where // slot_cap, lax.rem(where, slot_cap), :, at]
            part = dot(flat_of(gc, k * step, step), rhs)
            value = part if value is None else value + part
        dact2[:, at] = value
        return carry

    arrived(mix_xy)
    mix_z = rs_z(0)
    lax.fori_loop(0, unit_steps, cot_act, 0)
    arrived(mix_z)
    middle = (x_one + rs_end(0)).astype(bf16)
    mid_ref[...] = middle.astype(f32)
    x_two = mid_ref[...]
    inv_two = lax.rsqrt(jnp.mean(x_two * x_two, axis=1, keepdims=True) + norm_eps)
    g2[r, z, x, core] = (x_two * inv_two * gain_two).astype(bf16)
    two_z = ag_z(g2, 2)
    arrived(two_z)
    two_xy = ag_xy(g2, 2)
    arrived(two_xy)
    two_c = ag_core(g2, 2)
    slots_arrived(0)
    arrived(two_c)

    def hidden_two(j, carry):
        at = pl.ds(pl.multiple_of(j * step, step), step)
        value = None
        for k in range(tiles):
            where = pick[k]
            rhs = slots_in[where // slot_cap, lax.rem(where, slot_cap), :, at]
            part = dot(flat_of(g2, k * step, step), rhs)
            value = part if value is None else value + part
        act, slope = gelu_both(value)
        act2[:, :, :, at] = act.astype(bf16).reshape(groups, 2, tok, step)
        dh2[:, :, :, at] = (dact2[:, at] * slope).astype(bf16).reshape(groups, 2, tok, step)
        return carry

    lax.fori_loop(0, unit_steps, hidden_two, 0)

    def in_slot(k):
        where = pick[k]
        return slots_in[where // slot_cap, lax.rem(where, slot_cap)]

    def out_slot(k):
        where = pick[tiles + k]
        return slots_out[where // slot_cap, lax.rem(where, slot_cap)]

    back_c = rs_core(1, dh2, in_slot)
    for j, (src, dst) in enumerate(((g2, n2_out), (act2, act_out), (dh2, dh_out))):
        cp = pltpu.make_async_copy(src, dst, out_sem.at[1 + j])
        cp.start()
        outs.append(cp)
    arrived(back_c)
    back_xy = rs_xy(1)
    last_c = rs_core(2, act2, out_slot)
    arrived(back_xy)
    back_z = rs_z(1)
    arrived(last_c)
    last_xy = rs_xy(2)
    arrived(back_z)
    gated = rs_end(1) * gain_two
    mean = jnp.mean(x_two * gated, axis=1, keepdims=True)
    grad_mid = (
        gout_ref[...].astype(f32) + inv_two * gated - x_two * inv_two * inv_two * inv_two * mean
    ).astype(bf16)
    gm[r, z, x, core] = grad_mid
    gmid_ref[...] = grad_mid.astype(f32)
    cot_one_z = ag_z(gm, 3)
    arrived(last_xy)
    last_z = rs_z(2)
    arrived(cot_one_z)
    cot_one_xy = ag_xy(gm, 3)
    arrived(last_z)
    hid_out[...] = (x_two + rs_end(2)).astype(bf16)
    arrived(cot_one_xy)
    cot_one_c = ag_core(gm, 3)
    arrived(cot_one_c)

    def hidden_grad(j, carry):
        at = pl.ds(pl.multiple_of(j * step, step), step)
        value = dot(flat_of(gm, 0, width), weights[1, :, at]) * slope1[:, at]
        dh1[:, :, :, at] = value.astype(bf16).reshape(groups, 2, tok, step)
        return carry

    lax.fori_loop(0, unit_steps, hidden_grad, 0)
    first_c = rs_core(3, dh1, in_rows)

    def weight_grad(m, left, right):
        rhs = right[...].reshape(all_tok, units)

        def tile(j, carry):
            at = pl.ds(pl.multiple_of(j * step, step), step)
            lhs = left[:, :, :, :, :, at].reshape(all_tok, step)
            to = pl.ds(j * (step // per), step // per)
            grads[m, to] = dot_tn(lhs, rhs).astype(bf16).reshape(step // per, per, units)
            return carry

        lax.fori_loop(0, width_steps, tile, 0)
        cp = pltpu.make_async_copy(grads.at[m], gr_out.at[:, m], out_sem.at[4 + m])
        cp.start()
        outs.append(cp)

    arrived(first_c)
    first_xy = rs_xy(3)
    weight_grad(1, gm, act1)
    arrived(first_xy)
    first_z = rs_z(3)
    weight_grad(0, g1, dh1)
    arrived(first_z)
    gated = rs_end(3) * gain_one
    mean = jnp.mean(x_one * gated, axis=1, keepdims=True)
    gtok_out[...] = (
        gmid_ref[...] + inv_one * gated - x_one * inv_one * inv_one * inv_one * mean
    ).astype(bf16)

    for cp in outs:
        cp.wait()
    for group in (
        one_z, cot_z, one_xy, cot_xy, one_c, cot_c, mix_c, mix_xy, mix_z, two_z, two_xy, two_c,
        back_c, back_xy, back_z, last_c, last_xy, last_z, cot_one_z, cot_one_xy, cot_one_c,
        first_c, first_xy, first_z,
    ):
        for cp in group:
            cp.wait_send()
    for mm, dr, cp in slot_copies:
        if dr > 0:
            cp.wait_send()
    a2a_part(0).wait_send()
    a2a_part(1).wait_send()


def middle_call(dims, pick, tokens, grad_out, gains, flat_in, flat_out, tile_in, tile_out):
    rows, zs, xs, tok, width, units, per, slot_cap, tiles = dims
    cols = zs * xs * 2
    total = rows * cols
    groups = rows * zs * xs
    all_tok = total * tok
    f32, bf16 = jnp.float32, jnp.bfloat16
    shape = jax.ShapeDtypeStruct
    vmem = pl.BlockSpec(memory_space=pltpu.VMEM)
    hbm = pl.BlockSpec(memory_space=pl.ANY)
    lane = (rows, zs, xs, 2, tok, width)
    others = rows * xs
    dma = pltpu.SemaphoreType.DMA
    buf = pltpu.VMEM
    return pl.pallas_call(
        functools.partial(middle_kernel, dims),
        in_specs=[pl.BlockSpec(memory_space=pltpu.SMEM), vmem, vmem, vmem, hbm, hbm, hbm, hbm],
        out_specs=[vmem, vmem] + [hbm] * 5,
        out_shape=[
            shape((tok, width), bf16),
            shape((tok, width), bf16),
            shape((total, 2, per, units), bf16),
            shape((groups, 2, tok, units), bf16),
            shape((groups, 2, tok, units), bf16),
            shape(lane, bf16),
            shape(lane, bf16),
        ],
        scratch_shapes=[
            buf((2,) + flat_in.shape, bf16),
            buf((2, rows, cols, per, units), bf16),
            buf((2, width, units), bf16),
            buf((rows,) + tile_in.shape[1:3] + (units,), bf16),
            buf((rows,) + tile_in.shape[1:3] + (units,), bf16),
            buf(lane, bf16),
            buf(lane, bf16),
            buf(lane, bf16),
            buf(lane, bf16),
            buf((groups, 2, tok, units), bf16),
            buf((all_tok, units), f32),
            buf((all_tok, units), f32),
            buf((groups, 2, tok, units), bf16),
            buf((groups, 2, tok, units), bf16),
            buf((groups, 2, tok, units), bf16),
            buf((2, total, per, units), bf16),
            buf((4, groups, tok, width), bf16),
            buf((4, groups, tok, width), f32),
            buf((4, groups, tok, width), bf16),
            buf((4, rows, zs, xs, tok, width), bf16),
            buf((4, others, zs, tok, width), bf16),
            buf((4, zs, tok, width), bf16),
            buf((4, zs, tok, width), bf16),
            buf((tok, width), f32),
            buf((tok, width), f32),
            dma((2,)),
            dma((2,)),
            dma((2,)),
            dma((2,)),
            dma((2, rows)),
            dma((2, rows)),
            dma((4, zs + others)),
            dma((4, zs + others)),
            dma((4, zs + others)),
            dma((4, zs + others)),
            dma((6,)),
        ],
        compiler_params=pltpu.CompilerParams(
            has_side_effects=True, vmem_limit_bytes=63 * 1024 * 1024
        ),
        cost_estimate=pl.CostEstimate(
            flops=24 * all_tok * width * units, bytes_accessed=24 * width * units, transcendentals=0
        ),
        name="middle",
    )(pick, tokens, grad_out, gains, flat_in, flat_out, tile_in, tile_out)


def flat_both_kernel(cols, g, w_in, w_out, mom, sec, o_in, o_out, o_mom, o_sec):
    rows_in, width = cols * 16, g.shape[-1]
    p = lax.broadcasted_iota(jnp.int32, (rows_in, rows_in), 0)
    q = lax.broadcasted_iota(jnp.int32, (rows_in, rows_in), 1)
    swap = (lax.rem(p, cols) == q // 16) & (p // cols == lax.rem(q, 16))
    swap = jnp.where(swap, 1.0, 0.0).astype(jnp.bfloat16)
    for m, (w, o) in enumerate(((w_in, o_in), (w_out, o_out))):
        got = g[0, :, m].reshape(rows_in, width)
        grad = jnp.dot(swap, got, preferred_element_type=jnp.float32)
        o[...], o_mom[m], o_sec[m] = adam_update(w[...], grad, mom[m], sec[m])


def flat_both(w_in, w_out, g, mom, sec, dims):
    rows, zs, xs, tok, width, units, per, slot_cap, tiles = dims
    cols = zs * xs * 2
    rows_in = cols * 16
    step = min(units, 512)
    parts = units // step
    grid = (per // 16, rows * parts)
    thin = pl.BlockSpec((rows_in, step), lambda i, j: (i, j))
    wide = pl.BlockSpec((2, rows_in, step), lambda i, j: (0, i, j))
    got = pl.BlockSpec((1, cols, 2, 16, step), lambda i, j: (j // parts, 0, 0, i, j % parts))
    shape = jax.ShapeDtypeStruct
    return pl.pallas_call(
        functools.partial(flat_both_kernel, cols),
        grid=grid,
        in_specs=[got, thin, thin, wide, wide],
        out_specs=[thin, thin, wide, wide],
        out_shape=[
            shape(w_in.shape, w_in.dtype),
            shape(w_out.shape, w_out.dtype),
            shape(mom.shape, mom.dtype),
            shape(sec.shape, sec.dtype),
        ],
        cost_estimate=pl.CostEstimate(
            flops=30 * mom.size, bytes_accessed=22 * mom.size, transcendentals=2 * mom.size
        ),
        name="flat_both",
    )(g.reshape(rows, cols, 2, per, units), w_in, w_out, mom, sec)


def slot_kernel(
    tiles, live, l_in, l_out, r_in, r_out, w_in, w_out, mom, sec, o_in, o_out, o_mom, o_sec
):
    slot = pl.program_id(0)
    step = w_in.shape[-1]
    units = r_in.shape[-1]
    at = pl.program_id(1) * step
    row, lane = at // units, pl.multiple_of(lax.rem(at, units), step)
    parts = ((l_in, r_in, w_in, o_in), (l_out, r_out, w_out, o_out))
    for m, (left, right, w, o) in enumerate(parts):
        grad = dot_tn(left[...], right[row, :, pl.ds(lane, step)])
        alive = live[m, slot] > 0
        old_w, old_m, old_s = w[0, 0], mom[m, 0, 0], sec[m, 0, 0]
        new_w, new_m, new_s = adam_update(old_w, grad, old_m, old_s)
        o[0, 0] = jnp.where(alive, new_w.astype(jnp.float32), old_w.astype(jnp.float32)).astype(
            jnp.bfloat16
        )
        o_mom[m, 0, 0] = jnp.where(alive, new_m, old_m)
        o_sec[m, 0, 0] = jnp.where(alive, new_s, old_s)


def slot_adam(tiles, live, l_in, l_out, r_in, r_out, w_in, w_out, mom, sec):
    slot_cap, tile_rows, width = w_in.shape[1:]
    toks = l_in.shape[0]
    step = min(r_in.shape[-1], 512)

    def left_map(m):
        return lambda s, h, tiles, live: (0, tiles[m, s])

    def thin_map(s, h, *unused):
        return (0, s, 0, h)

    def wide_map(s, h, *unused):
        return (0, 0, s, 0, h)

    right = pl.BlockSpec(r_in.shape, lambda s, h, *unused: (0, 0, 0))
    thin = pl.BlockSpec((1, 1, tile_rows, step), thin_map)
    wide = pl.BlockSpec((2, 1, 1, tile_rows, step), wide_map)
    shape = jax.ShapeDtypeStruct
    return pl.pallas_call(
        slot_kernel,
        grid_spec=pltpu.PrefetchScalarGridSpec(
            num_scalar_prefetch=2,
            grid=(slot_cap, width // step),
            in_specs=[
                pl.BlockSpec((toks, tile_rows), left_map(0)),
                pl.BlockSpec((toks, tile_rows), left_map(1)),
                right,
                right,
                thin,
                thin,
                wide,
                wide,
            ],
            out_specs=[thin, thin, wide, wide],
        ),
        out_shape=[
            shape(w_in.shape, w_in.dtype),
            shape(w_out.shape, w_out.dtype),
            shape(mom.shape, mom.dtype),
            shape(sec.shape, sec.dtype),
        ],
        cost_estimate=pl.CostEstimate(
            flops=2 * toks * mom.size, bytes_accessed=22 * mom.size, transcendentals=mom.size
        ),
        name="slot_adam",
    )(tiles, live, l_in, l_out, r_in, r_out, w_in, w_out, mom, sec)


def fused_dims(row_total, col_total, tokens, flat_in, tile_in, owners):
    depth = 4 if col_total % 8 == 0 else 1
    across = col_total // (2 * depth)
    total = row_total * col_total
    tok, width = tokens.shape
    units = flat_in.shape[1] // row_total
    per = width // total
    slot_cap, tile_rows = tile_in.shape[1:3]
    tiles = owners.shape[-1]
    fits = (
        col_total % 2 == 0
        and width % total == 0
        and tok % 16 == 0
        and per % 16 == 0
        and units % 256 == 0
        and tile_rows == 256
        and tiles * tile_rows == width
        and total * tok * (width * 30 + units * 16) + width * units * 24 < 60 * 2**20
    )
    return (row_total, depth, across, tok, width, units, per, slot_cap, tiles) if fits else None


def fused_shards(
    dims,
    tokens,
    grad_out,
    gains,
    flat_in,
    flat_out,
    flat_moment,
    flat_second,
    tile_in,
    tile_out,
    tile_moment,
    tile_second,
    owners,
):
    rows, zs, xs, tok, width, units, per, slot_cap, tiles = dims
    cols = zs * xs * 2
    all_tok = rows * cols * tok
    row_index = lax.axis_index("row")
    owner_rows = owners[:, 0, :]
    ranks = tile_ranks(owner_rows)
    pick = (owner_rows * slot_cap + ranks).reshape(-1).astype(jnp.int32)
    slot_ids = jnp.arange(slot_cap, dtype=jnp.int32)[None, :, None]
    mine = (owner_rows == row_index)[:, None, :] & (ranks[:, None, :] == slot_ids)
    positions = jnp.arange(tiles, dtype=jnp.int32)
    my_tiles = jnp.sum(jnp.where(mine, positions, 0), axis=-1).astype(jnp.int32)
    my_live = jnp.any(mine, axis=-1).astype(jnp.int32)

    hidden_out, grad_tokens, grads, act, d_hidden, normed, cot = middle_call(
        dims, pick, tokens, grad_out, gains, flat_in, flat_out, tile_in, tile_out
    )
    act = act.reshape(all_tok, units)
    d_hidden = d_hidden.reshape(all_tok, units)

    def by_row(value):
        got = [value]
        for shift in range(1, rows):
            pairs = [(src, (src + shift) % rows) for src in range(rows)]
            got.append(lax.ppermute(value, "row", pairs))
        ids = [lax.rem(row_index - shift + rows, rows) for shift in range(rows)]
        if rows == 2:
            first = row_index == 0
            return jnp.stack([jnp.where(first, got[0], got[1]), jnp.where(first, got[1], got[0])])
        placed = jnp.zeros((rows,) + value.shape, value.dtype)
        for where, piece in zip(ids, got):
            placed = lax.dynamic_update_index_in_dim(placed, piece, where, 0)
        return placed

    act_rows = by_row(act)
    d_hidden_rows = by_row(d_hidden)

    def spread(grad):
        return lax.all_to_all(grad, both, split_axis=0, concat_axis=0, tiled=True)

    pair = spread(grads.reshape(rows * cols, 2 * per, units))
    new_tile = slot_adam(
        my_tiles,
        my_live,
        normed.reshape(all_tok, width),
        cot.reshape(all_tok, width),
        d_hidden_rows,
        act_rows,
        tile_in,
        tile_out,
        tile_moment,
        tile_second,
    )
    new_in, new_out, moment, second = flat_both(
        flat_in, flat_out, pair, flat_moment, flat_second, dims
    )
    return (hidden_out, grad_tokens, new_in, new_out, moment, second, *new_tile)


def solution(mesh):
    return jax.shard_map(
        shards,
        mesh=mesh,
        in_specs=(
            P(("row", "col"), None),
            P(("row", "col"), None),
            P(),
            P(("row", "col"), None),
            P(("row", "col"), None),
            P(None, ("row", "col"), None),
            P(None, ("row", "col"), None),
            P("col", "row", None, None),
            P("col", "row", None, None),
            P(None, "col", "row", None, None),
            P(None, "col", "row", None, None),
            P(None, "col", None),
        ),
        out_specs=(
            P(("row", "col"), None),
            P(("row", "col"), None),
            P(("row", "col"), None),
            P(("row", "col"), None),
            P(None, ("row", "col"), None),
            P(None, ("row", "col"), None),
            P("col", "row", None, None),
            P("col", "row", None, None),
            P(None, "col", "row", None, None),
            P(None, "col", "row", None, None),
        ),
        check_vma=False,
    )
```

```python
import functools

import jax
import jax.numpy as jnp
from jax import lax
from jax.experimental import pallas as pl
from jax.experimental.pallas import tpu as pltpu
from jax.sharding import PartitionSpec as P

norm_eps = 1e-06
beta_one = 0.9
beta_two = 0.95
learn_rate = 0.002
decay_rate = 0.1
adam_eps = 1e-08
gelu_coef = 0.7978845608
both = ("row", "col")


def gelu_both(hidden):
    square = hidden * hidden
    tanh_term = jnp.tanh(gelu_coef * (hidden + 0.044715 * square * hidden))
    value = 0.5 * hidden * (1.0 + tanh_term)
    slope = 0.5 * (1.0 + tanh_term) + 0.5 * hidden * (1.0 - tanh_term * tanh_term) * gelu_coef * (
        1.0 + 0.134145 * square
    )
    return value, slope


def adam_update(weight, gradient, moment, second):
    new_moment = beta_one * moment + (1.0 - beta_one) * gradient
    new_second = beta_two * second + (1.0 - beta_two) * gradient * gradient
    weight_float = weight.astype(jnp.float32)
    stepped = weight_float - learn_rate * (
        new_moment / (new_second * lax.rsqrt(new_second) + adam_eps) + decay_rate * weight_float
    )
    return (stepped.astype(jnp.bfloat16), new_moment, new_second)


def tile_ranks(owner_rows):
    positions = jnp.arange(owner_rows.shape[-1], dtype=jnp.int32)
    same_owner = owner_rows[..., :, None] == owner_rows[..., None, :]
    earlier = positions[None, :] < positions[:, None]
    return jnp.sum(jnp.where(same_owner & earlier, 1, 0), axis=-1).astype(jnp.int32)


def flat_kernel(w_in, w_out, g_in, g_out, mom, sec, o_in, o_out, o_mom, o_sec):
    for m, (w, g, o) in enumerate(((w_in, g_in, o_in), (w_out, g_out, o_out))):
        new = adam_update(w[...], g[...].astype(jnp.float32), mom[m], sec[m])
        o[...], o_mom[m], o_sec[m] = new


def flat_adam(w_in, w_out, g_in, g_out, mom, sec):
    rows, width = w_in.shape
    step = min(rows, 32)
    thin = pl.BlockSpec((step, width), lambda i: (i, 0))
    wide = pl.BlockSpec((2, step, width), lambda i: (0, i, 0))
    shape = jax.ShapeDtypeStruct
    return pl.pallas_call(
        flat_kernel,
        grid=(rows // step,),
        in_specs=[thin, thin, thin, thin, wide, wide],
        out_specs=[thin, thin, wide, wide],
        out_shape=[
            shape(w_in.shape, w_in.dtype),
            shape(w_out.shape, w_out.dtype),
            shape(mom.shape, mom.dtype),
            shape(sec.shape, sec.dtype),
        ],
        cost_estimate=pl.CostEstimate(
            flops=30 * mom.size, bytes_accessed=20 * mom.size + 2 * mom.size, transcendentals=mom.size
        ),
        name="flat_adam",
    )(w_in, w_out, g_in, g_out, mom, sec)


def tile_kernel(
    tiles, live, me, l_in, l_out, r_in, r_out, w_in, w_out, mom, sec, o_in, o_out, o_mom, o_sec
):
    slot = pl.program_id(0)
    parts = ((l_in, r_in, w_in, o_in), (l_out, r_out, w_out, o_out))
    for m, (left, right, w, o) in enumerate(parts):
        grad = jnp.dot(left[...], right[0], preferred_element_type=jnp.float32)
        alive = live[m, slot] > 0
        old_w, old_m, old_s = w[0, 0], mom[m, 0, 0], sec[m, 0, 0]
        new_w, new_m, new_s = adam_update(old_w, grad, old_m, old_s)
        o[0, 0] = jnp.where(alive, new_w.astype(jnp.float32), old_w.astype(jnp.float32)).astype(
            jnp.bfloat16
        )
        o_mom[m, 0, 0] = jnp.where(alive, new_m, old_m)
        o_sec[m, 0, 0] = jnp.where(alive, new_s, old_s)


def tile_adam(tiles, live, me, l_in, l_out, r_in, r_out, w_in, w_out, mom, sec):
    slot_cap, tile_rows, width = w_in.shape[1:]
    ranks, toks, sub = r_in.shape
    step = min(sub, 512)
    per = sub // step

    def left_map(m):
        return lambda s, h, tiles, live, me: (tiles[m, s], 0)

    def right_map(s, h, tiles, live, me):
        return (lax.rem(me[0] + ranks - h // per, ranks), 0, h % per)

    def thin_map(s, h, *unused):
        return (0, s, 0, h)

    def wide_map(s, h, *unused):
        return (0, 0, s, 0, h)

    right = pl.BlockSpec((1, toks, step), right_map)
    thin = pl.BlockSpec((1, 1, tile_rows, step), thin_map)
    wide = pl.BlockSpec((2, 1, 1, tile_rows, step), wide_map)
    shape = jax.ShapeDtypeStruct
    return pl.pallas_call(
        tile_kernel,
        grid_spec=pltpu.PrefetchScalarGridSpec(
            num_scalar_prefetch=3,
            grid=(slot_cap, width // step),
            in_specs=[
                pl.BlockSpec((tile_rows, toks), left_map(0)),
                pl.BlockSpec((tile_rows, toks), left_map(1)),
                right,
                right,
                thin,
                thin,
                wide,
                wide,
            ],
            out_specs=[thin, thin, wide, wide],
        ),
        out_shape=[
            shape(w_in.shape, w_in.dtype),
            shape(w_out.shape, w_out.dtype),
            shape(mom.shape, mom.dtype),
            shape(sec.shape, sec.dtype),
        ],
        cost_estimate=pl.CostEstimate(
            flops=2 * toks * mom.size, bytes_accessed=22 * mom.size, transcendentals=mom.size
        ),
        name="tile_adam",
    )(tiles, live, me, l_in, l_out, r_in, r_out, w_in, w_out, mom, sec)


def row_swap(pieces_for, row_total):
    got = [pieces_for(0)]
    for shift in range(1, row_total):
        pairs = [(src, (src + shift) % row_total) for src in range(row_total)]
        got.append(lax.ppermute(pieces_for(shift), "row", pairs))
    return jnp.stack(got)


def spread_sum(partial, total):
    toks, width = partial.shape
    sent = partial.astype(jnp.bfloat16)
    came = lax.all_to_all(sent, both, split_axis=0, concat_axis=0, tiled=True)
    return jnp.sum(came.reshape(total, toks // total, width).astype(jnp.float32), axis=0)


def late_sum(partial):
    return lax.psum_scatter(
        partial.astype(jnp.bfloat16), both, scatter_dimension=0, tiled=True
    ).astype(jnp.float32)


def dot_nt(left, right):
    return lax.dot_general(left, right, (((1,), (1,)), ((), ())), preferred_element_type=jnp.float32)


def dot_tn(left, right):
    return lax.dot_general(left, right, (((0,), (0,)), ((), ())), preferred_element_type=jnp.float32)


def norm_of(layer_in, gain_vec):
    tok_float = layer_in.astype(jnp.float32)
    inv_rms = lax.rsqrt(jnp.mean(tok_float * tok_float, axis=1, keepdims=True) + norm_eps)
    normed = (tok_float * inv_rms * gain_vec).astype(jnp.bfloat16)
    return tok_float, inv_rms, normed


def token_grad(cotangent, d_normed, gain_vec, tok_float, inv_rms):
    gated = d_normed * gain_vec
    return (
        cotangent.astype(jnp.float32)
        + inv_rms * gated
        - tok_float
        * inv_rms
        * inv_rms
        * inv_rms
        * jnp.mean(tok_float * gated, axis=1, keepdims=True)
    ).astype(jnp.bfloat16)


def shards(
    tokens,
    grad_out,
    gains,
    flat_in,
    flat_out,
    flat_moment,
    flat_second,
    tile_in,
    tile_out,
    tile_moment,
    tile_second,
    owners,
):
    row_total = lax.axis_size("row")
    col_total = lax.axis_size("col")
    dims = fused_dims(row_total, col_total, tokens, flat_in, tile_in, owners)
    if dims is not None:
        return fused_shards(
            dims,
            tokens,
            grad_out,
            gains,
            flat_in,
            flat_out,
            flat_moment,
            flat_second,
            tile_in,
            tile_out,
            tile_moment,
            tile_second,
            owners,
        )
    total = row_total * col_total
    row_index = lax.axis_index("row")
    model_width = tokens.shape[1]
    block = flat_in.shape[1]
    sub = block // row_total
    own_rows = flat_in.shape[0] // col_total
    slot_cap = tile_in.shape[1]
    tile_rows = tile_in.shape[2]

    owner_rows = owners[:, 0, :]
    ranks = tile_ranks(owner_rows)
    came_from = lax.rem(row_index - owner_rows + row_total, row_total)
    slot_pick = came_from * slot_cap + ranks
    slots = jnp.arange(slot_cap, dtype=jnp.int32)[None, :, None]
    mine = (owner_rows == row_index)[:, None, :] & (ranks[:, None, :] == slots)
    positions = jnp.arange(owner_rows.shape[1], dtype=jnp.int32)
    my_tiles = jnp.sum(jnp.where(mine, positions, 0), axis=-1).astype(jnp.int32)
    my_live = jnp.any(mine, axis=-1).astype(jnp.int32)

    def flat_to_units(flat):
        parts = flat.reshape(own_rows, col_total, row_total, sub).transpose(2, 1, 0, 3)
        return lax.all_to_all(
            parts.reshape(total * own_rows, sub), both, split_axis=0, concat_axis=0, tiled=True
        )

    def units_to_flat(grad):
        came = lax.all_to_all(
            grad.astype(jnp.bfloat16), both, split_axis=0, concat_axis=0, tiled=True
        )
        parts = came.reshape(row_total, col_total, own_rows, sub).transpose(2, 1, 0, 3)
        return parts.reshape(own_rows * col_total, block)

    def tiles_to_units(tile, pick):
        def piece(shift):
            to_row = lax.rem(row_index + shift, row_total)
            return lax.dynamic_slice_in_dim(tile[0], to_row * sub, sub, 2)

        whole = row_swap(piece, row_total).reshape(row_total * slot_cap, tile_rows, sub)
        return jnp.take(whole, pick, axis=0).reshape(model_width, sub)

    def gather(x):
        return lax.all_gather(x, both, axis=0, tiled=True)

    tok_one, inv_one, normed_one = norm_of(tokens, gains[0])
    normed_one = gather(normed_one)
    one_in = flat_to_units(flat_in)
    one_out = flat_to_units(flat_out)
    cot_two = gather(grad_out)
    two_in = tiles_to_units(tile_in, slot_pick[0])
    two_out = tiles_to_units(tile_out, slot_pick[1])
    hidden_one = jnp.dot(normed_one, one_in, preferred_element_type=jnp.float32)
    act_one, slope_one = gelu_both(hidden_one)
    act_one = act_one.astype(jnp.bfloat16)
    middle = (tok_one + spread_sum(dot_nt(act_one, one_out), total)).astype(jnp.bfloat16)

    tok_two, inv_two, normed_two = norm_of(middle, gains[1])
    normed_two = gather(normed_two)
    hidden_two = jnp.dot(normed_two, two_in, preferred_element_type=jnp.float32)
    act_two, slope_two = gelu_both(hidden_two)
    act_two = act_two.astype(jnp.bfloat16)
    d_act_two = jnp.dot(cot_two, two_out, preferred_element_type=jnp.float32)
    d_hidden_two = (d_act_two * slope_two).astype(jnp.bfloat16)
    d_normed_two = spread_sum(dot_nt(d_hidden_two, two_in), total)
    grad_mid = token_grad(grad_out, d_normed_two, gains[1], tok_two, inv_two)
    cot_one = gather(grad_mid)

    d_act_one = jnp.dot(cot_one, one_out, preferred_element_type=jnp.float32)
    d_hidden_one = (d_act_one * slope_one).astype(jnp.bfloat16)
    flat_grad_in = units_to_flat(dot_tn(normed_one, d_hidden_one))
    flat_grad_out = units_to_flat(dot_tn(cot_one, act_one))

    act_late, _ = lax.optimization_barrier((act_two, cot_one))
    mixed_two = late_sum(dot_nt(act_late, two_out))
    hidden_out = (tok_two + mixed_two).astype(jnp.bfloat16)
    d_normed_one = late_sum(dot_nt(d_hidden_one, one_in))
    grad_tokens = token_grad(grad_mid, d_normed_one, gains[0], tok_one, inv_one)

    d_hidden_rows = row_swap(lambda shift: d_hidden_two, row_total)
    act_rows = row_swap(lambda shift: act_two, row_total)
    new_tile = tile_adam(
        my_tiles,
        my_live,
        row_index.astype(jnp.int32).reshape(1),
        normed_two.T,
        cot_two.T,
        d_hidden_rows,
        act_rows,
        tile_in,
        tile_out,
        tile_moment,
        tile_second,
    )
    new_flat = flat_adam(flat_in, flat_out, flat_grad_in, flat_grad_out, flat_moment, flat_second)
    return (hidden_out, grad_tokens, *new_flat, *new_tile)


MESH = pl.DeviceIdType.MESH


def middle_kernel(
    dims,
    pick,
    tok_ref,
    gout_ref,
    gains_ref,
    flat_in,
    flat_out,
    tile_in,
    tile_out,
    hid_out,
    gtok_out,
    gr_out,
    act_out,
    dh_out,
    n2_out,
    c2_out,
    stage,
    send,
    weights,
    slots_in,
    own_out,
    cot_send,
    cot_far,
    g1,
    gc,
    g2,
    gm,
    act1,
    slope1,
    dact2,
    act2,
    act2_far,
    dh2,
    dh1,
    grads,
    psend,
    pown,
    rcore,
    s1,
    rxy,
    s2,
    rz,
    mid_ref,
    gmid_ref,
    stage_sem,
    a2a_send,
    a2a_recv,
    slot_local,
    slot_send,
    slot_recv,
    ag_send,
    ag_recv,
    rs_send,
    rs_recv,
    act_send,
    act_recv,
    cot_ssem,
    cot_rsem,
    out_sem,
):
    rows, zs, xs, tok, width, units, per, slot_cap, tiles = dims
    cols = zs * xs * 2
    total = rows * cols
    groups = rows * zs * xs
    all_tok = total * tok
    step = 256
    unit_steps = units // step
    width_steps = width // step
    r = lax.axis_index("row")
    c = lax.axis_index("col")
    me = r * cols + c
    core = lax.rem(c, 2)
    x = lax.rem(c // 2, xs)
    z = c // (2 * xs)
    f32, bf16 = jnp.float32, jnp.bfloat16

    def col_of(zi, xi, ci):
        return (zi * xs + xi) * 2 + ci

    def remote(src, dst, ssem, rsem, row_to, col_to):
        return pltpu.make_async_remote_copy(
            src_ref=src,
            dst_ref=dst,
            send_sem=ssem,
            recv_sem=rsem,
            device_id=(row_to, col_to),
            device_id_type=MESH,
        )

    sent = []
    plane = [(dr, dx) for dr in range(rows) for dx in range(xs) if (dr, dx) != (0, 0)]

    def ag_z(g, n):
        out = []
        for dz in range(1, zs):
            zt = lax.rem(z + dz, zs)
            here = g.at[r, z, x, core]
            out.append(
                remote(here, here, ag_send.at[n, dz], ag_recv.at[n, dz], r, col_of(zt, x, core))
            )
        for cp in out:
            cp.start()
        sent.extend(out)
        return out

    def ag_xy(g, n):
        out = []
        for j, (dr, dx) in enumerate(plane):
            rt, xt = lax.rem(r + dr, rows), lax.rem(x + dx, xs)
            here = g.at[r, :, x, core]
            out.append(
                remote(
                    here,
                    here,
                    ag_send.at[n, zs + j],
                    ag_recv.at[n, zs + j],
                    rt,
                    col_of(z, xt, core),
                )
            )
        for cp in out:
            cp.start()
        sent.extend(out)
        return out

    def ag_core(g, n):
        here = g.at[:, :, :, core]
        cp = remote(here, here, ag_send.at[n, 0], ag_recv.at[n, 0], r, col_of(z, x, 1 - core))
        cp.start()
        sent.append(cp)
        return [cp]

    def arrived(copies):
        for cp in copies:
            cp.wait_recv()

    def flat_of(g, lo, size):
        return g[:, :, :, :, :, lo : lo + size].reshape(all_tok, size)

    def dot(a, b):
        return jnp.dot(a, b, preferred_element_type=f32)

    def rs_core(n, lhs, rhs, own=None):
        def half(which, store):
            left = [lh[:, pl.ds(which, 1)].reshape(groups * tok, units) for lh in lhs]

            def tile(j, carry):
                at = pl.ds(pl.multiple_of(j * step, step), step)
                value = None
                for lh, rh in zip(left, rhs):
                    part = dot_nt(lh, rh(j))
                    value = part if value is None else value + part
                if own is not None:
                    value = jnp.where(own(j), value, 0.0)
                store(at, value.reshape(groups, tok, step))
                return carry

            lax.fori_loop(0, width_steps, tile, 0)

        def to_send(at, value):
            psend[n, :, :, at] = value.astype(bf16)

        def to_own(at, value):
            pown[n, :, :, at] = value

        half(1 - core, to_send)
        cp = remote(
            psend.at[n], rcore.at[n], rs_send.at[n, 0], rs_recv.at[n, 0], r, col_of(z, x, 1 - core)
        )
        cp.start()
        sent.append(cp)
        half(core, to_own)
        return [cp]

    def rs_xy(n):
        def add(k, carry):
            value = pown[n, k] + rcore[n, k].astype(f32)
            s1[n, k // (zs * xs), lax.rem(k // xs, zs), lax.rem(k, xs)] = value.astype(bf16)
            return carry

        lax.fori_loop(0, groups, add, 0)
        out = []
        for j, (dr, dx) in enumerate(plane):
            rt, xt = lax.rem(r + dr, rows), lax.rem(x + dx, xs)
            out.append(
                remote(
                    s1.at[n, rt, :, xt],
                    rxy.at[n, j],
                    rs_send.at[n, 1 + j],
                    rs_recv.at[n, 1 + j],
                    rt,
                    col_of(z, xt, core),
                )
            )
        for cp in out:
            cp.start()
        sent.extend(out)
        return out

    def rs_z(n):
        def add(k, carry):
            value = s1[n, r, k, x].astype(f32)
            for j in range(len(plane)):
                value = value + rxy[n, j, k].astype(f32)
            s2[n, k] = value.astype(bf16)
            return carry

        lax.fori_loop(0, zs, add, 0)
        out = []
        for dz in range(1, zs):
            zt = lax.rem(z + dz, zs)
            j = len(plane) + dz
            out.append(
                remote(
                    s2.at[n, zt],
                    rz.at[n, dz],
                    rs_send.at[n, j],
                    rs_recv.at[n, j],
                    r,
                    col_of(zt, x, core),
                )
            )
        for cp in out:
            cp.start()
        sent.extend(out)
        return out

    def rs_end(n):
        value = s2[n, z].astype(f32)
        for dz in range(1, zs):
            value = value + rz[n, dz].astype(f32)
        return value

    def a2a_start(m, first):
        def one(k, carry):
            to = lax.rem(me + k, total)
            rt, ct = to // cols, lax.rem(to, cols)
            at = pl.ds(pl.multiple_of(me * per, per), per)
            remote(send.at[m, rt, ct], weights.at[m, at], a2a_send.at[m], a2a_recv.at[m], rt, ct).start()
            return carry

        lax.fori_loop(first, total, one, 0)

    def a2a_part(m):
        span = weights.at[m, pl.ds(0, (total - 1) * per)]
        return remote(span, span, a2a_send.at[m], a2a_recv.at[m], r, c)

    def permute(m):
        rows_in = cols * 16
        p = lax.broadcasted_iota(jnp.int32, (rows_in, rows_in), 0)
        q = lax.broadcasted_iota(jnp.int32, (rows_in, rows_in), 1)
        swap = (lax.rem(p, 16) == q // cols) & (p // 16 == lax.rem(q, cols))
        swap = jnp.where(swap, 1.0, 0.0).astype(bf16)

        wide = min(units, 512)

        def block(k, carry):
            b, h = k // (units // wide), lax.rem(k, units // wide)
            from_rows = pl.ds(pl.multiple_of(b * rows_in, rows_in), rows_in)
            to_rows = pl.ds(pl.multiple_of(b * 16, 16), 16)
            to_lanes = pl.ds(pl.multiple_of(h * wide, wide), wide)
            for rt in range(rows):
                lanes = pl.ds(pl.multiple_of(rt * units + h * wide, wide), wide)
                got = dot(swap, stage[m, from_rows, lanes]).astype(bf16).reshape(cols, 16, wide)
                send[m, rt, :, to_rows, to_lanes] = got
            return carry

        lax.fori_loop(0, (per // 16) * (units // wide), block, 0)
        weights[m, pl.ds(pl.multiple_of(me * per, per), per), :] = send[m, r, c]

    loads = [
        pltpu.make_async_copy(flat, stage.at[m], stage_sem.at[m])
        for m, flat in enumerate((flat_in, flat_out))
    ]
    for cp in loads:
        cp.start()

    slot_copies = []
    half_rows = slots_in.shape[2] // 2
    my_lanes = pl.ds(pl.multiple_of(r * units, units), units)
    slot_loads = [
        pltpu.make_async_copy(tile_in.at[0, :, :, my_lanes], slots_in.at[r], slot_local.at[0]),
        pltpu.make_async_copy(tile_out.at[0], own_out, slot_local.at[1]),
    ]
    for cp in slot_loads:
        cp.start()

    def lanes_of(dr):
        return pl.ds(pl.multiple_of(lax.rem(r + dr, rows) * units, units), units)

    def slots_start(first, last):
        for q in range(first, last):
            slot, part = q // 2, pl.ds(q % 2 * half_rows, half_rows)
            for dr in range(1, rows):
                cp = remote(
                    tile_in.at[0, slot, part, lanes_of(dr)],
                    slots_in.at[r, slot, part],
                    slot_send.at[dr, q],
                    slot_recv.at[dr, q],
                    lax.rem(r + dr, rows),
                    c,
                )
                sent.append(cp)
                cp.start()
                slot_copies.append(cp)

    x_one = tok_ref[...].astype(f32)
    inv_one = lax.rsqrt(jnp.mean(x_one * x_one, axis=1, keepdims=True) + norm_eps)
    gain_one = gains_ref[0:1, :]
    gain_two = gains_ref[1:2, :]
    g1[r, z, x, core] = (x_one * inv_one * gain_one).astype(bf16)
    gc[r, z, x, core] = gout_ref[...]
    one_z = ag_z(g1, 0)
    cot_z = ag_z(gc, 1)
    slots_start(0, 1)
    loads[0].wait()
    permute(0)
    arrived(one_z)
    one_xy = ag_xy(g1, 0)
    arrived(cot_z)
    cot_xy = ag_xy(gc, 1)
    a2a_start(0, 1)
    slots_start(1, 2 * slot_cap)
    loads[1].wait()
    permute(1)
    a2a_start(1, 1)
    arrived(one_xy)
    one_c = ag_core(g1, 0)
    arrived(cot_xy)
    cot_c = ag_core(gc, 1)

    arrived(one_c)
    arrived(cot_c)
    outs = []
    for j, (src, dst) in enumerate(((gc, c2_out),)):
        cp = pltpu.make_async_copy(src, dst, out_sem.at[0])
        cp.start()
        outs.append(cp)

    slot_loads[1].wait()

    def cot_tile(store, lanes0, j):
        value = None
        for k in range(tiles):
            flag = jnp.where(pick[2 * tiles + k] > 0, 1.0, 0.0).astype(bf16)
            lanes = pl.ds(pl.multiple_of(lanes0 + j * step, step), step)
            part = dot(flat_of(gc, k * step, step), own_out[pick[tiles + k], :, lanes] * flag)
            value = part if value is None else value + part
        store(pl.ds(pl.multiple_of(j * step, step), step), value)

    cot_copies = []
    for dr in range(1, rows):

        def cot_other(j, carry, dr=dr):
            def store(at, value):
                cot_send[dr - 1, :, at] = value.astype(bf16)

            cot_tile(store, lax.rem(r + dr, rows) * units, j)
            return carry

        lax.fori_loop(0, unit_steps, cot_other, 0)
        cp = remote(
            cot_send.at[dr - 1],
            cot_far.at[dr - 1],
            cot_ssem.at[dr],
            cot_rsem.at[dr],
            lax.rem(r + dr, rows),
            c,
        )
        cp.start()
        sent.append(cp)
        cot_copies.append(cp)

    def cot_mine(j, carry):
        def store(at, value):
            dact2[:, at] = value

        cot_tile(store, r * units, j)
        return carry

    lax.fori_loop(0, unit_steps, cot_mine, 0)

    a2a_part(0).wait_recv()

    def hidden_one(j, carry):
        at = pl.ds(pl.multiple_of(j * step, step), step)
        act, slope = gelu_both(dot(flat_of(g1, 0, width), weights[0, :, at]))
        act1[:, :, :, at] = act.astype(bf16).reshape(groups, 2, tok, step)
        slope1[:, at] = slope
        return carry

    lax.fori_loop(0, unit_steps, hidden_one, 0)
    a2a_part(1).wait_recv()

    def out_rows(j):
        return weights[1, pl.ds(pl.multiple_of(j * step, step), step), :]

    def in_rows(j):
        return weights[0, pl.ds(pl.multiple_of(j * step, step), step), :]

    mix_c = rs_core(0, [act1], [out_rows])
    arrived(mix_c)
    mix_xy = rs_xy(0)

    arrived(mix_xy)
    mix_z = rs_z(0)
    arrived(mix_z)
    middle = (x_one + rs_end(0)).astype(bf16)
    mid_ref[...] = middle.astype(f32)
    x_two = mid_ref[...]
    inv_two = lax.rsqrt(jnp.mean(x_two * x_two, axis=1, keepdims=True) + norm_eps)
    g2[r, z, x, core] = (x_two * inv_two * gain_two).astype(bf16)

    two_z = ag_z(g2, 2)
    arrived(two_z)
    two_xy = ag_xy(g2, 2)
    arrived(two_xy)
    two_c = ag_core(g2, 2)
    slot_loads[0].wait()
    arrived(slot_copies)
    arrived(cot_copies)
    arrived(two_c)

    def hidden_two(j, carry):
        at = pl.ds(pl.multiple_of(j * step, step), step)
        value = None
        for k in range(tiles):
            where = pick[k]
            rhs = slots_in[where // slot_cap, lax.rem(where, slot_cap), :, at]
            part = dot(flat_of(g2, k * step, step), rhs)
            value = part if value is None else value + part
        act, slope = gelu_both(value)
        act2[:, :, :, at] = act.astype(bf16).reshape(groups, 2, tok, step)
        d_act = dact2[:, at]
        for dr in range(1, rows):
            d_act = d_act + cot_far[dr - 1, :, at].astype(f32)
        dh2[:, :, :, at] = (d_act * slope).astype(bf16).reshape(groups, 2, tok, step)
        return carry

    lax.fori_loop(0, unit_steps, hidden_two, 0)

    def in_slot(k):
        where = pick[k]
        return slots_in[where // slot_cap, lax.rem(where, slot_cap)]

    act_copies = []
    piece = groups // 4

    def act_start(q):
        for dr in range(1, rows):
            span = pl.ds(q * piece, piece)
            cp = remote(
                act2.at[span],
                act2_far.at[dr - 1, span],
                act_send.at[dr, q],
                act_recv.at[dr, q],
                lax.rem(r + dr, rows),
                c,
            )
            cp.start()
            sent.append(cp)
            act_copies.append(cp)

    act_start(0)
    act_start(1)
    back_c = rs_core(1, [dh2], [in_slot])
    for j, (src, dst) in enumerate(((g2, n2_out), (act2, act_out.at[r]), (dh2, dh_out))):
        cp = pltpu.make_async_copy(src, dst, out_sem.at[1 + j])
        cp.start()
        outs.append(cp)
    arrived(back_c)
    back_xy = rs_xy(1)
    arrived(back_xy)
    back_z = rs_z(1)
    act_start(2)
    act_start(3)
    arrived(back_z)
    gated = rs_end(1) * gain_two
    mean = jnp.mean(x_two * gated, axis=1, keepdims=True)
    grad_mid = (
        gout_ref[...].astype(f32) + inv_two * gated - x_two * inv_two * inv_two * inv_two * mean
    ).astype(bf16)
    gm[r, z, x, core] = grad_mid
    gmid_ref[...] = grad_mid.astype(f32)
    cot_one_z = ag_z(gm, 3)
    arrived(cot_one_z)
    cot_one_xy = ag_xy(gm, 3)

    def out_slot(dr):
        return lambda k: own_out[pick[tiles + k], :, lanes_of(dr)]

    def mine(k):
        return pick[2 * tiles + k] > 0

    arrived(act_copies)
    last_c = rs_core(
        2,
        [act2] + [act2_far.at[dr - 1] for dr in range(1, rows)],
        [out_slot((rows - dr) % rows) for dr in range(rows)],
        mine,
    )
    arrived(cot_one_xy)
    cot_one_c = ag_core(gm, 3)
    for dr in range(1, rows):
        cp = pltpu.make_async_copy(
            act2_far.at[dr - 1], act_out.at[lax.rem(r + rows - dr, rows)], out_sem.at[5 + dr]
        )
        cp.start()
        outs.append(cp)
    arrived(last_c)
    last_xy = rs_xy(2)
    arrived(cot_one_c)

    def hidden_grad(j, carry):
        at = pl.ds(pl.multiple_of(j * step, step), step)
        value = dot(flat_of(gm, 0, width), weights[1, :, at]) * slope1[:, at]
        dh1[:, :, :, at] = value.astype(bf16).reshape(groups, 2, tok, step)
        return carry

    lax.fori_loop(0, unit_steps, hidden_grad, 0)
    first_c = rs_core(3, [dh1], [in_rows])

    def weight_grad(m, left, right):
        rhs = right[...].reshape(all_tok, units)

        def tile(j, carry):
            at = pl.ds(pl.multiple_of(j * step, step), step)
            lhs = left[:, :, :, :, :, at].reshape(all_tok, step)
            to = pl.ds(j * (step // per), step // per)
            grads[m, to] = dot_tn(lhs, rhs).astype(bf16).reshape(step // per, per, units)
            return carry

        lax.fori_loop(0, width_steps, tile, 0)
        cp = pltpu.make_async_copy(grads.at[m], gr_out.at[:, m], out_sem.at[4 + m])
        cp.start()
        outs.append(cp)

    arrived(last_xy)
    last_z = rs_z(2)
    arrived(first_c)
    first_xy = rs_xy(3)
    weight_grad(1, gm, act1)
    arrived(last_z)
    hid_out[...] = (x_two + rs_end(2)).astype(bf16)
    arrived(first_xy)
    first_z = rs_z(3)
    weight_grad(0, g1, dh1)
    arrived(first_z)
    gated = rs_end(3) * gain_one
    mean = jnp.mean(x_one * gated, axis=1, keepdims=True)
    gtok_out[...] = (
        gmid_ref[...] + inv_one * gated - x_one * inv_one * inv_one * inv_one * mean
    ).astype(bf16)

    for cp in outs:
        cp.wait()
    for cp in sent:
        cp.wait_send()
    a2a_part(0).wait_send()
    a2a_part(1).wait_send()


def middle_call(dims, pick, tokens, grad_out, gains, flat_in, flat_out, tile_in, tile_out):
    rows, zs, xs, tok, width, units, per, slot_cap, tiles = dims
    cols = zs * xs * 2
    total = rows * cols
    groups = rows * zs * xs
    all_tok = total * tok
    f32, bf16 = jnp.float32, jnp.bfloat16
    shape = jax.ShapeDtypeStruct
    vmem = pl.BlockSpec(memory_space=pltpu.VMEM)
    hbm = pl.BlockSpec(memory_space=pl.ANY)
    lane = (rows, zs, xs, 2, tok, width)
    others = rows * xs
    dma = pltpu.SemaphoreType.DMA
    buf = pltpu.VMEM
    return pl.pallas_call(
        functools.partial(middle_kernel, dims),
        in_specs=[pl.BlockSpec(memory_space=pltpu.SMEM), vmem, vmem, vmem, hbm, hbm, hbm, hbm],
        out_specs=[vmem, vmem] + [hbm] * 5,
        out_shape=[
            shape((tok, width), bf16),
            shape((tok, width), bf16),
            shape((total, 2, per, units), bf16),
            shape((rows, groups, 2, tok, units), bf16),
            shape((groups, 2, tok, units), bf16),
            shape(lane, bf16),
            shape(lane, bf16),
        ],
        scratch_shapes=[
            buf((2,) + flat_in.shape, bf16),
            buf((2, rows, cols, per, units), bf16),
            buf((2, width, units), bf16),
            buf((rows,) + tile_in.shape[1:3] + (units,), bf16),
            buf(tile_out.shape[1:], bf16),
            buf((rows - 1, all_tok, units), bf16),
            buf((rows - 1, all_tok, units), bf16),
            buf(lane, bf16),
            buf(lane, bf16),
            buf(lane, bf16),
            buf(lane, bf16),
            buf((groups, 2, tok, units), bf16),
            buf((all_tok, units), f32),
            buf((all_tok, units), f32),
            buf((groups, 2, tok, units), bf16),
            buf((rows - 1, groups, 2, tok, units), bf16),
            buf((groups, 2, tok, units), bf16),
            buf((groups, 2, tok, units), bf16),
            buf((2, total, per, units), bf16),
            buf((4, groups, tok, width), bf16),
            buf((4, groups, tok, width), f32),
            buf((4, groups, tok, width), bf16),
            buf((4, rows, zs, xs, tok, width), bf16),
            buf((4, others, zs, tok, width), bf16),
            buf((4, zs, tok, width), bf16),
            buf((4, zs, tok, width), bf16),
            buf((tok, width), f32),
            buf((tok, width), f32),
            dma((2,)),
            dma((2,)),
            dma((2,)),
            dma((2,)),
            dma((rows, 2 * slot_cap)),
            dma((rows, 2 * slot_cap)),
            dma((4, zs + others)),
            dma((4, zs + others)),
            dma((4, zs + others)),
            dma((4, zs + others)),
            dma((rows, 4)),
            dma((rows, 4)),
            dma((rows,)),
            dma((rows,)),
            dma((6 + rows,)),
        ],
        compiler_params=pltpu.CompilerParams(
            has_side_effects=True, vmem_limit_bytes=63 * 1024 * 1024
        ),
        cost_estimate=pl.CostEstimate(
            flops=24 * all_tok * width * units, bytes_accessed=24 * width * units, transcendentals=0
        ),
        name="middle",
    )(pick, tokens, grad_out, gains, flat_in, flat_out, tile_in, tile_out)


def flat_both_kernel(cols, split, g, w_in, w_out, mom, sec, o_in, o_out, o_mom, o_sec):
    rows, units = g.shape[0], g.shape[-1]
    rows_in = cols * 16
    part = rows_in // split
    p = lax.broadcasted_iota(jnp.int32, (part, rows_in), 0) + pl.program_id(1) * part
    q = lax.broadcasted_iota(jnp.int32, (part, rows_in), 1)
    swap = (lax.rem(p, cols) == q // 16) & (p // cols == lax.rem(q, 16))
    swap = jnp.where(swap, 1.0, 0.0).astype(jnp.bfloat16)
    for m, (w, o) in enumerate(((w_in, o_in), (w_out, o_out))):
        for rt in range(rows):
            at = slice(rt * units, (rt + 1) * units)
            got = g[rt, :, m].reshape(rows_in, units)
            grad = jnp.dot(swap, got, preferred_element_type=jnp.float32)
            new = adam_update(w[:, at], grad, mom[m, :, at], sec[m, :, at])
            o[:, at], o_mom[m, :, at], o_sec[m, :, at] = new


def flat_both(w_in, w_out, g, mom, sec, dims):
    rows, zs, xs, tok, width, units, per, slot_cap, tiles = dims
    cols = zs * xs * 2
    split = 2
    part = cols * 16 // split
    block = rows * units
    thin = pl.BlockSpec((part, block), lambda i, h: (i * split + h, 0))
    wide = pl.BlockSpec((2, part, block), lambda i, h: (0, i * split + h, 0))
    got = pl.BlockSpec((rows, cols, 2, 16, units), lambda i, h: (0, 0, 0, i, 0))
    shape = jax.ShapeDtypeStruct
    return pl.pallas_call(
        functools.partial(flat_both_kernel, cols, split),
        grid=(per // 16, split),
        in_specs=[got, thin, thin, wide, wide],
        out_specs=[thin, thin, wide, wide],
        out_shape=[
            shape(w_in.shape, w_in.dtype),
            shape(w_out.shape, w_out.dtype),
            shape(mom.shape, mom.dtype),
            shape(sec.shape, sec.dtype),
        ],
        cost_estimate=pl.CostEstimate(
            flops=30 * mom.size, bytes_accessed=22 * mom.size, transcendentals=2 * mom.size
        ),
        name="flat_both",
    )(g.reshape(rows, cols, 2, per, units), w_in, w_out, mom, sec)


def slot_kernel_part(m, tiles, live, left, right, w, mom, sec, *rest):
    o, o_mom, o_sec = rest[-3:]
    slot = pl.program_id(0)
    step = w.shape[-1]
    units = right.shape[-1]
    at = pl.program_id(1) * step
    row, lane = at // units, pl.multiple_of(lax.rem(at, units), step)
    grad = dot_tn(left[...], right[row, :, pl.ds(lane, step)])
    alive = live[m, slot] > 0
    old_w, old_m, old_s = w[0, 0], mom[0, 0, 0], sec[0, 0, 0]
    new_w, new_m, new_s = adam_update(old_w, grad, old_m, old_s)
    o[0, 0] = jnp.where(alive, new_w.astype(jnp.float32), old_w.astype(jnp.float32)).astype(
        jnp.bfloat16
    )
    o_mom[0, 0, 0] = jnp.where(alive, new_m, old_m)
    o_sec[0, 0, 0] = jnp.where(alive, new_s, old_s)


def slot_part(m, tiles, live, left, right, w, mom, sec, before=()):
    slot_cap, tile_rows, width = w.shape[1:]
    toks = left.shape[0]
    step = min(right.shape[-1], 1024)
    thin = pl.BlockSpec((1, 1, tile_rows, step), lambda s, h, *unused: (0, s, 0, h))
    wide = pl.BlockSpec((1, 1, 1, tile_rows, step), lambda s, h, *unused: (m, 0, s, 0, h))
    shape = jax.ShapeDtypeStruct
    return pl.pallas_call(
        functools.partial(slot_kernel_part, m),
        grid_spec=pltpu.PrefetchScalarGridSpec(
            num_scalar_prefetch=2,
            grid=(slot_cap, width // step),
            in_specs=[
                pl.BlockSpec((toks, tile_rows), lambda s, h, tiles, live: (0, tiles[m, s])),
                pl.BlockSpec(right.shape, lambda s, h, *unused: (0, 0, 0)),
                thin,
                wide,
                wide,
            ]
            + [pl.BlockSpec(memory_space=pl.ANY)] * len(before),
            out_specs=[thin, wide, wide],
        ),
        out_shape=[
            shape(w.shape, w.dtype),
            shape(mom.shape, mom.dtype),
            shape(sec.shape, sec.dtype),
        ],
        input_output_aliases={7 + i: 1 + i for i in range(len(before))},
        cost_estimate=pl.CostEstimate(
            flops=10**10, bytes_accessed=22 * w.size, transcendentals=2 * w.size
        ),
        name="slot_part",
    )(tiles, live, left, right, w, mom, sec, *before)


def fused_dims(row_total, col_total, tokens, flat_in, tile_in, owners):
    depth = 4 if col_total % 8 == 0 else 1
    across = col_total // (2 * depth)
    total = row_total * col_total
    tok, width = tokens.shape
    units = flat_in.shape[1] // row_total
    per = width // total
    slot_cap, tile_rows = tile_in.shape[1:3]
    tiles = owners.shape[-1]
    fits = (
        col_total % 2 == 0
        and width % total == 0
        and tok % 16 == 0
        and per % 16 == 0
        and units % 256 == 0
        and tile_rows == 256
        and tiles * tile_rows == width
        and total * tok * (width * 30 + units * 16) + width * units * 24 < 60 * 2**20
    )
    return (row_total, depth, across, tok, width, units, per, slot_cap, tiles) if fits else None


def fused_shards(
    dims,
    tokens,
    grad_out,
    gains,
    flat_in,
    flat_out,
    flat_moment,
    flat_second,
    tile_in,
    tile_out,
    tile_moment,
    tile_second,
    owners,
):
    rows, zs, xs, tok, width, units, per, slot_cap, tiles = dims
    cols = zs * xs * 2
    all_tok = rows * cols * tok
    row_index = lax.axis_index("row")
    owner_rows = owners[:, 0, :]
    ranks = tile_ranks(owner_rows)
    owned = (owner_rows == row_index).astype(jnp.int32)
    slot_of = owner_rows[0] * slot_cap + ranks[0]
    pick = jnp.concatenate([slot_of, ranks[1] * owned[1], owned[1]]).astype(jnp.int32)
    slot_ids = jnp.arange(slot_cap, dtype=jnp.int32)[None, :, None]
    mine = (owner_rows == row_index)[:, None, :] & (ranks[:, None, :] == slot_ids)
    positions = jnp.arange(tiles, dtype=jnp.int32)
    my_tiles = jnp.sum(jnp.where(mine, positions, 0), axis=-1).astype(jnp.int32)
    my_live = jnp.any(mine, axis=-1).astype(jnp.int32)

    hidden_out, grad_tokens, grads, act, d_hidden, normed, cot = middle_call(
        dims, pick, tokens, grad_out, gains, flat_in, flat_out, tile_in, tile_out
    )
    act_rows = act.reshape(rows, all_tok, units)
    d_hidden = d_hidden.reshape(all_tok, units)

    def by_row(value):
        got = [value]
        for shift in range(1, rows):
            pairs = [(src, (src + shift) % rows) for src in range(rows)]
            got.append(lax.ppermute(value, "row", pairs))
        ids = [lax.rem(row_index - shift + rows, rows) for shift in range(rows)]
        if rows == 2:
            first = row_index == 0
            return jnp.stack([jnp.where(first, got[0], got[1]), jnp.where(first, got[1], got[0])])
        placed = jnp.zeros((rows,) + value.shape, value.dtype)
        for where, piece in zip(ids, got):
            placed = lax.dynamic_update_index_in_dim(placed, piece, where, 0)
        return placed

    d_hidden_rows = by_row(d_hidden)

    def spread(grad):
        return lax.all_to_all(grad, both, split_axis=0, concat_axis=0, tiled=True)

    pair = spread(grads.reshape(rows * cols, 2 * per, units))
    tile_w_out, tile_m, tile_s = slot_part(
        1, my_tiles, my_live, cot.reshape(all_tok, width), act_rows, tile_out, tile_moment, tile_second
    )
    tile_w_in, tile_m, tile_s = slot_part(
        0,
        my_tiles,
        my_live,
        normed.reshape(all_tok, width),
        d_hidden_rows,
        tile_in,
        tile_moment,
        tile_second,
        (tile_m, tile_s),
    )
    new_in, new_out, moment, second = flat_both(
        flat_in, flat_out, pair, flat_moment, flat_second, dims
    )
    new_tile = (tile_w_in, tile_w_out, tile_m, tile_s)
    return (hidden_out, grad_tokens, new_in, new_out, moment, second, *new_tile)


def solution(mesh):
    return jax.shard_map(
        shards,
        mesh=mesh,
        in_specs=(
            P(("row", "col"), None),
            P(("row", "col"), None),
            P(),
            P(("row", "col"), None),
            P(("row", "col"), None),
            P(None, ("row", "col"), None),
            P(None, ("row", "col"), None),
            P("col", "row", None, None),
            P("col", "row", None, None),
            P(None, "col", "row", None, None),
            P(None, "col", "row", None, None),
            P(None, "col", None),
        ),
        out_specs=(
            P(("row", "col"), None),
            P(("row", "col"), None),
            P(("row", "col"), None),
            P(("row", "col"), None),
            P(None, ("row", "col"), None),
            P(None, ("row", "col"), None),
            P("col", "row", None, None),
            P("col", "row", None, None),
            P(None, "col", "row", None, None),
            P(None, "col", "row", None, None),
        ),
        check_vma=False,
    )
```

```python
import functools

import jax
import jax.numpy as jnp
from jax import lax
from jax.experimental import pallas as pl
from jax.experimental.pallas import tpu as pltpu
from jax.sharding import PartitionSpec as P

norm_eps = 1e-06
beta_one = 0.9
beta_two = 0.95
learn_rate = 0.002
decay_rate = 0.1
adam_eps = 1e-08
gelu_coef = 0.7978845608
both = ("row", "col")


def gelu_both(hidden):
    square = hidden * hidden
    tanh_term = jnp.tanh(gelu_coef * (hidden + 0.044715 * square * hidden))
    value = 0.5 * hidden * (1.0 + tanh_term)
    slope = 0.5 * (1.0 + tanh_term) + 0.5 * hidden * (1.0 - tanh_term * tanh_term) * gelu_coef * (
        1.0 + 0.134145 * square
    )
    return value, slope


def adam_update(weight, gradient, moment, second):
    new_moment = beta_one * moment + (1.0 - beta_one) * gradient
    new_second = beta_two * second + (1.0 - beta_two) * gradient * gradient
    weight_float = weight.astype(jnp.float32)
    stepped = weight_float - learn_rate * (
        new_moment / (new_second * lax.rsqrt(new_second) + adam_eps) + decay_rate * weight_float
    )
    return (stepped.astype(jnp.bfloat16), new_moment, new_second)


def tile_ranks(owner_rows):
    positions = jnp.arange(owner_rows.shape[-1], dtype=jnp.int32)
    same_owner = owner_rows[..., :, None] == owner_rows[..., None, :]
    earlier = positions[None, :] < positions[:, None]
    return jnp.sum(jnp.where(same_owner & earlier, 1, 0), axis=-1).astype(jnp.int32)


def flat_kernel(w_in, w_out, g_in, g_out, mom, sec, o_in, o_out, o_mom, o_sec):
    for m, (w, g, o) in enumerate(((w_in, g_in, o_in), (w_out, g_out, o_out))):
        new = adam_update(w[...], g[...].astype(jnp.float32), mom[m], sec[m])
        o[...], o_mom[m], o_sec[m] = new


def flat_adam(w_in, w_out, g_in, g_out, mom, sec):
    rows, width = w_in.shape
    step = min(rows, 32)
    thin = pl.BlockSpec((step, width), lambda i: (i, 0))
    wide = pl.BlockSpec((2, step, width), lambda i: (0, i, 0))
    shape = jax.ShapeDtypeStruct
    return pl.pallas_call(
        flat_kernel,
        grid=(rows // step,),
        in_specs=[thin, thin, thin, thin, wide, wide],
        out_specs=[thin, thin, wide, wide],
        out_shape=[
            shape(w_in.shape, w_in.dtype),
            shape(w_out.shape, w_out.dtype),
            shape(mom.shape, mom.dtype),
            shape(sec.shape, sec.dtype),
        ],
        cost_estimate=pl.CostEstimate(
            flops=30 * mom.size, bytes_accessed=20 * mom.size + 2 * mom.size, transcendentals=mom.size
        ),
        name="flat_adam",
    )(w_in, w_out, g_in, g_out, mom, sec)


def tile_kernel(
    tiles, live, me, l_in, l_out, r_in, r_out, w_in, w_out, mom, sec, o_in, o_out, o_mom, o_sec
):
    slot = pl.program_id(0)
    parts = ((l_in, r_in, w_in, o_in), (l_out, r_out, w_out, o_out))
    for m, (left, right, w, o) in enumerate(parts):
        grad = jnp.dot(left[...], right[0], preferred_element_type=jnp.float32)
        alive = live[m, slot] > 0
        old_w, old_m, old_s = w[0, 0], mom[m, 0, 0], sec[m, 0, 0]
        new_w, new_m, new_s = adam_update(old_w, grad, old_m, old_s)
        o[0, 0] = jnp.where(alive, new_w.astype(jnp.float32), old_w.astype(jnp.float32)).astype(
            jnp.bfloat16
        )
        o_mom[m, 0, 0] = jnp.where(alive, new_m, old_m)
        o_sec[m, 0, 0] = jnp.where(alive, new_s, old_s)


def tile_adam(tiles, live, me, l_in, l_out, r_in, r_out, w_in, w_out, mom, sec):
    slot_cap, tile_rows, width = w_in.shape[1:]
    ranks, toks, sub = r_in.shape
    step = min(sub, 512)
    per = sub // step

    def left_map(m):
        return lambda s, h, tiles, live, me: (tiles[m, s], 0)

    def right_map(s, h, tiles, live, me):
        return (lax.rem(me[0] + ranks - h // per, ranks), 0, h % per)

    def thin_map(s, h, *unused):
        return (0, s, 0, h)

    def wide_map(s, h, *unused):
        return (0, 0, s, 0, h)

    right = pl.BlockSpec((1, toks, step), right_map)
    thin = pl.BlockSpec((1, 1, tile_rows, step), thin_map)
    wide = pl.BlockSpec((2, 1, 1, tile_rows, step), wide_map)
    shape = jax.ShapeDtypeStruct
    return pl.pallas_call(
        tile_kernel,
        grid_spec=pltpu.PrefetchScalarGridSpec(
            num_scalar_prefetch=3,
            grid=(slot_cap, width // step),
            in_specs=[
                pl.BlockSpec((tile_rows, toks), left_map(0)),
                pl.BlockSpec((tile_rows, toks), left_map(1)),
                right,
                right,
                thin,
                thin,
                wide,
                wide,
            ],
            out_specs=[thin, thin, wide, wide],
        ),
        out_shape=[
            shape(w_in.shape, w_in.dtype),
            shape(w_out.shape, w_out.dtype),
            shape(mom.shape, mom.dtype),
            shape(sec.shape, sec.dtype),
        ],
        cost_estimate=pl.CostEstimate(
            flops=2 * toks * mom.size, bytes_accessed=22 * mom.size, transcendentals=mom.size
        ),
        name="tile_adam",
    )(tiles, live, me, l_in, l_out, r_in, r_out, w_in, w_out, mom, sec)


def row_swap(pieces_for, row_total):
    got = [pieces_for(0)]
    for shift in range(1, row_total):
        pairs = [(src, (src + shift) % row_total) for src in range(row_total)]
        got.append(lax.ppermute(pieces_for(shift), "row", pairs))
    return jnp.stack(got)


def spread_sum(partial, total):
    toks, width = partial.shape
    sent = partial.astype(jnp.bfloat16)
    came = lax.all_to_all(sent, both, split_axis=0, concat_axis=0, tiled=True)
    return jnp.sum(came.reshape(total, toks // total, width).astype(jnp.float32), axis=0)


def late_sum(partial):
    return lax.psum_scatter(
        partial.astype(jnp.bfloat16), both, scatter_dimension=0, tiled=True
    ).astype(jnp.float32)


def dot_nt(left, right):
    return lax.dot_general(left, right, (((1,), (1,)), ((), ())), preferred_element_type=jnp.float32)


def dot_tn(left, right):
    return lax.dot_general(left, right, (((0,), (0,)), ((), ())), preferred_element_type=jnp.float32)


def norm_of(layer_in, gain_vec):
    tok_float = layer_in.astype(jnp.float32)
    inv_rms = lax.rsqrt(jnp.mean(tok_float * tok_float, axis=1, keepdims=True) + norm_eps)
    normed = (tok_float * inv_rms * gain_vec).astype(jnp.bfloat16)
    return tok_float, inv_rms, normed


def token_grad(cotangent, d_normed, gain_vec, tok_float, inv_rms):
    gated = d_normed * gain_vec
    return (
        cotangent.astype(jnp.float32)
        + inv_rms * gated
        - tok_float
        * inv_rms
        * inv_rms
        * inv_rms
        * jnp.mean(tok_float * gated, axis=1, keepdims=True)
    ).astype(jnp.bfloat16)


def shards(
    tokens,
    grad_out,
    gains,
    flat_in,
    flat_out,
    flat_moment,
    flat_second,
    tile_in,
    tile_out,
    tile_moment,
    tile_second,
    owners,
):
    row_total = lax.axis_size("row")
    col_total = lax.axis_size("col")
    dims = fused_dims(row_total, col_total, tokens, flat_in, tile_in, owners)
    if dims is not None:
        return fused_shards(
            dims,
            tokens,
            grad_out,
            gains,
            flat_in,
            flat_out,
            flat_moment,
            flat_second,
            tile_in,
            tile_out,
            tile_moment,
            tile_second,
            owners,
        )
    total = row_total * col_total
    row_index = lax.axis_index("row")
    model_width = tokens.shape[1]
    block = flat_in.shape[1]
    sub = block // row_total
    own_rows = flat_in.shape[0] // col_total
    slot_cap = tile_in.shape[1]
    tile_rows = tile_in.shape[2]

    owner_rows = owners[:, 0, :]
    ranks = tile_ranks(owner_rows)
    came_from = lax.rem(row_index - owner_rows + row_total, row_total)
    slot_pick = came_from * slot_cap + ranks
    slots = jnp.arange(slot_cap, dtype=jnp.int32)[None, :, None]
    mine = (owner_rows == row_index)[:, None, :] & (ranks[:, None, :] == slots)
    positions = jnp.arange(owner_rows.shape[1], dtype=jnp.int32)
    my_tiles = jnp.sum(jnp.where(mine, positions, 0), axis=-1).astype(jnp.int32)
    my_live = jnp.any(mine, axis=-1).astype(jnp.int32)

    def flat_to_units(flat):
        parts = flat.reshape(own_rows, col_total, row_total, sub).transpose(2, 1, 0, 3)
        return lax.all_to_all(
            parts.reshape(total * own_rows, sub), both, split_axis=0, concat_axis=0, tiled=True
        )

    def units_to_flat(grad):
        came = lax.all_to_all(
            grad.astype(jnp.bfloat16), both, split_axis=0, concat_axis=0, tiled=True
        )
        parts = came.reshape(row_total, col_total, own_rows, sub).transpose(2, 1, 0, 3)
        return parts.reshape(own_rows * col_total, block)

    def tiles_to_units(tile, pick):
        def piece(shift):
            to_row = lax.rem(row_index + shift, row_total)
            return lax.dynamic_slice_in_dim(tile[0], to_row * sub, sub, 2)

        whole = row_swap(piece, row_total).reshape(row_total * slot_cap, tile_rows, sub)
        return jnp.take(whole, pick, axis=0).reshape(model_width, sub)

    def gather(x):
        return lax.all_gather(x, both, axis=0, tiled=True)

    tok_one, inv_one, normed_one = norm_of(tokens, gains[0])
    normed_one = gather(normed_one)
    one_in = flat_to_units(flat_in)
    one_out = flat_to_units(flat_out)
    cot_two = gather(grad_out)
    two_in = tiles_to_units(tile_in, slot_pick[0])
    two_out = tiles_to_units(tile_out, slot_pick[1])
    hidden_one = jnp.dot(normed_one, one_in, preferred_element_type=jnp.float32)
    act_one, slope_one = gelu_both(hidden_one)
    act_one = act_one.astype(jnp.bfloat16)
    middle = (tok_one + spread_sum(dot_nt(act_one, one_out), total)).astype(jnp.bfloat16)

    tok_two, inv_two, normed_two = norm_of(middle, gains[1])
    normed_two = gather(normed_two)
    hidden_two = jnp.dot(normed_two, two_in, preferred_element_type=jnp.float32)
    act_two, slope_two = gelu_both(hidden_two)
    act_two = act_two.astype(jnp.bfloat16)
    d_act_two = jnp.dot(cot_two, two_out, preferred_element_type=jnp.float32)
    d_hidden_two = (d_act_two * slope_two).astype(jnp.bfloat16)
    d_normed_two = spread_sum(dot_nt(d_hidden_two, two_in), total)
    grad_mid = token_grad(grad_out, d_normed_two, gains[1], tok_two, inv_two)
    cot_one = gather(grad_mid)

    d_act_one = jnp.dot(cot_one, one_out, preferred_element_type=jnp.float32)
    d_hidden_one = (d_act_one * slope_one).astype(jnp.bfloat16)
    flat_grad_in = units_to_flat(dot_tn(normed_one, d_hidden_one))
    flat_grad_out = units_to_flat(dot_tn(cot_one, act_one))

    act_late, _ = lax.optimization_barrier((act_two, cot_one))
    mixed_two = late_sum(dot_nt(act_late, two_out))
    hidden_out = (tok_two + mixed_two).astype(jnp.bfloat16)
    d_normed_one = late_sum(dot_nt(d_hidden_one, one_in))
    grad_tokens = token_grad(grad_mid, d_normed_one, gains[0], tok_one, inv_one)

    d_hidden_rows = row_swap(lambda shift: d_hidden_two, row_total)
    act_rows = row_swap(lambda shift: act_two, row_total)
    new_tile = tile_adam(
        my_tiles,
        my_live,
        row_index.astype(jnp.int32).reshape(1),
        normed_two.T,
        cot_two.T,
        d_hidden_rows,
        act_rows,
        tile_in,
        tile_out,
        tile_moment,
        tile_second,
    )
    new_flat = flat_adam(flat_in, flat_out, flat_grad_in, flat_grad_out, flat_moment, flat_second)
    return (hidden_out, grad_tokens, *new_flat, *new_tile)


MESH = pl.DeviceIdType.MESH


def middle_kernel(
    dims,
    pick,
    tok_ref,
    gout_ref,
    gains_ref,
    flat_in,
    flat_out,
    tile_in,
    tile_out,
    hid_out,
    gtok_out,
    gr_out,
    act_out,
    dh_out,
    n2_out,
    c2_out,
    stage,
    send,
    weights,
    slots_in,
    own_out,
    cot_send,
    cot_far,
    g1,
    gc,
    g2,
    gm,
    act1,
    slope1,
    dact2,
    act2,
    act2_far,
    dh2,
    dh1,
    grads,
    psend,
    pown,
    rcore,
    s1,
    rxy,
    s2,
    rz,
    mid_ref,
    gmid_ref,
    stage_sem,
    a2a_send,
    a2a_recv,
    slot_local,
    slot_send,
    slot_recv,
    ag_send,
    ag_recv,
    rs_send,
    rs_recv,
    act_send,
    act_recv,
    cot_ssem,
    cot_rsem,
    out_sem,
):
    rows, zs, xs, tok, width, units, per, slot_cap, tiles = dims
    cols = zs * xs * 2
    total = rows * cols
    groups = rows * zs * xs
    all_tok = total * tok
    step = 256
    unit_steps = units // step
    width_steps = width // step
    r = lax.axis_index("row")
    c = lax.axis_index("col")
    me = r * cols + c
    core = lax.rem(c, 2)
    x = lax.rem(c // 2, xs)
    z = c // (2 * xs)
    f32, bf16 = jnp.float32, jnp.bfloat16

    def col_of(zi, xi, ci):
        return (zi * xs + xi) * 2 + ci

    def remote(src, dst, ssem, rsem, row_to, col_to):
        return pltpu.make_async_remote_copy(
            src_ref=src,
            dst_ref=dst,
            send_sem=ssem,
            recv_sem=rsem,
            device_id=(row_to, col_to),
            device_id_type=MESH,
        )

    sent = []
    plane = [(dr, dx) for dr in range(rows) for dx in range(xs) if (dr, dx) != (0, 0)]

    def ag_z(g, n):
        out = []
        for dz in range(1, zs):
            zt = lax.rem(z + dz, zs)
            here = g.at[r, z, x, core]
            out.append(
                remote(here, here, ag_send.at[n, dz], ag_recv.at[n, dz], r, col_of(zt, x, core))
            )
        for cp in out:
            cp.start()
        sent.extend(out)
        return out

    def ag_xy(g, n):
        out = []
        for j, (dr, dx) in enumerate(plane):
            rt, xt = lax.rem(r + dr, rows), lax.rem(x + dx, xs)
            here = g.at[r, :, x, core]
            out.append(
                remote(
                    here,
                    here,
                    ag_send.at[n, zs + j],
                    ag_recv.at[n, zs + j],
                    rt,
                    col_of(z, xt, core),
                )
            )
        for cp in out:
            cp.start()
        sent.extend(out)
        return out

    def ag_y(g, n):
        out = []
        for dr in range(1, rows):
            here = g.at[r, :, x, core]
            sems = ag_send.at[n, zs + dr - 1], ag_recv.at[n, zs + dr - 1]
            out.append(remote(here, here, *sems, lax.rem(r + dr, rows), col_of(z, x, core)))
        for cp in out:
            cp.start()
        sent.extend(out)
        return out

    def ag_x(g, n):
        out = []
        for dx in range(1, xs):
            here = g.at[:, :, x, core]
            j = zs + rows - 2 + dx
            xt = lax.rem(x + dx, xs)
            out.append(
                remote(here, here, ag_send.at[n, j], ag_recv.at[n, j], r, col_of(z, xt, core))
            )
        for cp in out:
            cp.start()
        sent.extend(out)
        return out

    def ag_core(g, n):
        here = g.at[:, :, :, core]
        cp = remote(here, here, ag_send.at[n, 0], ag_recv.at[n, 0], r, col_of(z, x, 1 - core))
        cp.start()
        sent.append(cp)
        return [cp]

    def arrived(copies):
        for cp in copies:
            cp.wait_recv()

    def flat_of(g, lo, size):
        return g[:, :, :, :, :, lo : lo + size].reshape(all_tok, size)

    def dot(a, b):
        return jnp.dot(a, b, preferred_element_type=f32)

    def rs_core(n, lhs, rhs, own=None):
        def half(which, store):
            left = [lh[:, pl.ds(which, 1)].reshape(groups * tok, units) for lh in lhs]

            def tile(j, carry):
                at = pl.ds(pl.multiple_of(j * step, step), step)
                value = None
                for lh, rh in zip(left, rhs):
                    part = dot_nt(lh, rh(j))
                    value = part if value is None else value + part
                if own is not None:
                    value = jnp.where(own(j), value, 0.0)
                store(at, value.reshape(groups, tok, step))
                return carry

            lax.fori_loop(0, width_steps, tile, 0)

        def to_send(at, value):
            psend[n, :, :, at] = value.astype(bf16)

        def to_own(at, value):
            pown[n, :, :, at] = value

        half(1 - core, to_send)
        cp = remote(
            psend.at[n], rcore.at[n], rs_send.at[n, 0], rs_recv.at[n, 0], r, col_of(z, x, 1 - core)
        )
        cp.start()
        sent.append(cp)
        half(core, to_own)
        return [cp]

    def rs_xy(n):
        def add(k, carry):
            value = pown[n, k] + rcore[n, k].astype(f32)
            s1[n, k // (zs * xs), lax.rem(k // xs, zs), lax.rem(k, xs)] = value.astype(bf16)
            return carry

        lax.fori_loop(0, groups, add, 0)
        out = []
        for j, (dr, dx) in enumerate(plane):
            rt, xt = lax.rem(r + dr, rows), lax.rem(x + dx, xs)
            out.append(
                remote(
                    s1.at[n, rt, :, xt],
                    rxy.at[n, j],
                    rs_send.at[n, 1 + j],
                    rs_recv.at[n, 1 + j],
                    rt,
                    col_of(z, xt, core),
                )
            )
        for cp in out:
            cp.start()
        sent.extend(out)
        return out

    def rs_z(n):
        def add(k, carry):
            value = s1[n, r, k, x].astype(f32)
            for j in range(len(plane)):
                value = value + rxy[n, j, k].astype(f32)
            s2[n, k] = value.astype(bf16)
            return carry

        lax.fori_loop(0, zs, add, 0)
        out = []
        for dz in range(1, zs):
            zt = lax.rem(z + dz, zs)
            j = len(plane) + dz
            out.append(
                remote(
                    s2.at[n, zt],
                    rz.at[n, dz],
                    rs_send.at[n, j],
                    rs_recv.at[n, j],
                    r,
                    col_of(zt, x, core),
                )
            )
        for cp in out:
            cp.start()
        sent.extend(out)
        return out

    def rs_end(n):
        value = s2[n, z].astype(f32)
        for dz in range(1, zs):
            value = value + rz[n, dz].astype(f32)
        return value

    def a2a_start(m, first):
        def one(k, carry):
            to = lax.rem(me + k, total)
            rt, ct = to // cols, lax.rem(to, cols)
            at = pl.ds(pl.multiple_of(me * per, per), per)
            remote(send.at[m, rt, ct], weights.at[m, at], a2a_send.at[m], a2a_recv.at[m], rt, ct).start()
            return carry

        lax.fori_loop(first, total, one, 0)

    def a2a_part(m):
        span = weights.at[m, pl.ds(0, (total - 1) * per)]
        return remote(span, span, a2a_send.at[m], a2a_recv.at[m], r, c)

    def permute(m):
        rows_in = cols * 16
        p = lax.broadcasted_iota(jnp.int32, (rows_in, rows_in), 0)
        q = lax.broadcasted_iota(jnp.int32, (rows_in, rows_in), 1)
        swap = (lax.rem(p, 16) == q // cols) & (p // 16 == lax.rem(q, cols))
        swap = jnp.where(swap, 1.0, 0.0).astype(bf16)

        wide = min(units, 512)

        def block(k, carry):
            b, h = k // (units // wide), lax.rem(k, units // wide)
            from_rows = pl.ds(pl.multiple_of(b * rows_in, rows_in), rows_in)
            to_rows = pl.ds(pl.multiple_of(b * 16, 16), 16)
            to_lanes = pl.ds(pl.multiple_of(h * wide, wide), wide)
            for rt in range(rows):
                lanes = pl.ds(pl.multiple_of(rt * units + h * wide, wide), wide)
                got = dot(swap, stage[m, from_rows, lanes]).astype(bf16).reshape(cols, 16, wide)
                send[m, rt, :, to_rows, to_lanes] = got
            return carry

        lax.fori_loop(0, (per // 16) * (units // wide), block, 0)
        weights[m, pl.ds(pl.multiple_of(me * per, per), per), :] = send[m, r, c]

    loads = [
        pltpu.make_async_copy(flat, stage.at[m], stage_sem.at[m])
        for m, flat in enumerate((flat_in, flat_out))
    ]
    for cp in loads:
        cp.start()

    slot_copies = []
    half_rows = slots_in.shape[2] // 2
    my_lanes = pl.ds(pl.multiple_of(r * units, units), units)
    slot_loads = [
        pltpu.make_async_copy(tile_in.at[0, :, :, my_lanes], slots_in.at[r], slot_local.at[0]),
        pltpu.make_async_copy(tile_out.at[0], own_out, slot_local.at[1]),
    ]
    for cp in slot_loads:
        cp.start()

    def lanes_of(dr):
        return pl.ds(pl.multiple_of(lax.rem(r + dr, rows) * units, units), units)

    def slots_start(first, last):
        for q in range(first, last):
            slot, part = q // 2, pl.ds(q % 2 * half_rows, half_rows)
            for dr in range(1, rows):
                cp = remote(
                    tile_in.at[0, slot, part, lanes_of(dr)],
                    slots_in.at[r, slot, part],
                    slot_send.at[dr, q],
                    slot_recv.at[dr, q],
                    lax.rem(r + dr, rows),
                    c,
                )
                sent.append(cp)
                cp.start()
                slot_copies.append(cp)

    x_one = tok_ref[...].astype(f32)
    inv_one = lax.rsqrt(jnp.mean(x_one * x_one, axis=1, keepdims=True) + norm_eps)
    gain_one = gains_ref[0:1, :]
    gain_two = gains_ref[1:2, :]
    g1[r, z, x, core] = (x_one * inv_one * gain_one).astype(bf16)
    gc[r, z, x, core] = gout_ref[...]
    one_z = ag_z(g1, 0)
    cot_z = ag_z(gc, 1)
    slots_start(0, 1)
    loads[0].wait()
    permute(0)
    arrived(one_z)
    one_y = ag_y(g1, 0)
    arrived(cot_z)
    cot_y = ag_y(gc, 1)
    a2a_start(0, 1)
    slots_start(1, 2 * slot_cap)
    loads[1].wait()
    permute(1)
    a2a_start(1, 1)
    arrived(cot_y)
    cot_x = ag_x(gc, 1)
    arrived(one_y)
    one_x = ag_x(g1, 0)
    arrived(cot_x)
    cot_c = ag_core(gc, 1)
    arrived(one_x)
    one_c = ag_core(g1, 0)

    arrived(one_c)
    arrived(cot_c)
    outs = []
    for j, (src, dst) in enumerate(((gc, c2_out),)):
        cp = pltpu.make_async_copy(src, dst, out_sem.at[0])
        cp.start()
        outs.append(cp)

    slot_loads[1].wait()

    def cot_tile(store, lanes0, j):
        value = None
        for k in range(tiles):
            flag = jnp.where(pick[2 * tiles + k] > 0, 1.0, 0.0).astype(bf16)
            lanes = pl.ds(pl.multiple_of(lanes0 + j * step, step), step)
            part = dot(flat_of(gc, k * step, step), own_out[pick[tiles + k], :, lanes] * flag)
            value = part if value is None else value + part
        store(pl.ds(pl.multiple_of(j * step, step), step), value)

    cot_copies = []
    for dr in range(1, rows):

        def cot_other(j, carry, dr=dr):
            def store(at, value):
                cot_send[dr - 1, :, at] = value.astype(bf16)

            cot_tile(store, lax.rem(r + dr, rows) * units, j)
            return carry

        lax.fori_loop(0, unit_steps, cot_other, 0)
        cp = remote(
            cot_send.at[dr - 1],
            cot_far.at[dr - 1],
            cot_ssem.at[dr],
            cot_rsem.at[dr],
            lax.rem(r + dr, rows),
            c,
        )
        cp.start()
        sent.append(cp)
        cot_copies.append(cp)

    def cot_mine(j, carry):
        def store(at, value):
            dact2[:, at] = value

        cot_tile(store, r * units, j)
        return carry

    lax.fori_loop(0, unit_steps, cot_mine, 0)

    a2a_part(0).wait_recv()

    def hidden_one(j, carry):
        at = pl.ds(pl.multiple_of(j * step, step), step)
        act, slope = gelu_both(dot(flat_of(g1, 0, width), weights[0, :, at]))
        act1[:, :, :, at] = act.astype(bf16).reshape(groups, 2, tok, step)
        slope1[:, at] = slope
        return carry

    lax.fori_loop(0, unit_steps, hidden_one, 0)
    a2a_part(1).wait_recv()

    def out_rows(j):
        return weights[1, pl.ds(pl.multiple_of(j * step, step), step), :]

    def in_rows(j):
        return weights[0, pl.ds(pl.multiple_of(j * step, step), step), :]

    mix_c = rs_core(0, [act1], [out_rows])
    arrived(mix_c)
    mix_xy = rs_xy(0)

    arrived(mix_xy)
    mix_z = rs_z(0)
    arrived(mix_z)
    middle = (x_one + rs_end(0)).astype(bf16)
    mid_ref[...] = middle.astype(f32)
    x_two = mid_ref[...]
    inv_two = lax.rsqrt(jnp.mean(x_two * x_two, axis=1, keepdims=True) + norm_eps)
    g2[r, z, x, core] = (x_two * inv_two * gain_two).astype(bf16)

    two_z = ag_z(g2, 2)
    arrived(two_z)
    two_xy = ag_xy(g2, 2)
    arrived(two_xy)
    two_c = ag_core(g2, 2)
    slot_loads[0].wait()
    arrived(slot_copies)
    arrived(cot_copies)
    arrived(two_c)

    def hidden_two(j, carry):
        at = pl.ds(pl.multiple_of(j * step, step), step)
        value = None
        for k in range(tiles):
            where = pick[k]
            rhs = slots_in[where // slot_cap, lax.rem(where, slot_cap), :, at]
            part = dot(flat_of(g2, k * step, step), rhs)
            value = part if value is None else value + part
        act, slope = gelu_both(value)
        act2[:, :, :, at] = act.astype(bf16).reshape(groups, 2, tok, step)
        d_act = dact2[:, at]
        for dr in range(1, rows):
            d_act = d_act + cot_far[dr - 1, :, at].astype(f32)
        dh2[:, :, :, at] = (d_act * slope).astype(bf16).reshape(groups, 2, tok, step)
        return carry

    lax.fori_loop(0, unit_steps, hidden_two, 0)

    def in_slot(k):
        where = pick[k]
        return slots_in[where // slot_cap, lax.rem(where, slot_cap)]

    act_copies = []
    piece = groups // 4

    def act_start(q):
        for dr in range(1, rows):
            span = pl.ds(q * piece, piece)
            cp = remote(
                act2.at[span],
                act2_far.at[dr - 1, span],
                act_send.at[dr, q],
                act_recv.at[dr, q],
                lax.rem(r + dr, rows),
                c,
            )
            cp.start()
            sent.append(cp)
            act_copies.append(cp)

    act_start(0)
    act_start(1)
    back_c = rs_core(1, [dh2], [in_slot])
    for j, (src, dst) in enumerate(((g2, n2_out), (act2, act_out.at[r]), (dh2, dh_out))):
        cp = pltpu.make_async_copy(src, dst, out_sem.at[1 + j])
        cp.start()
        outs.append(cp)
    arrived(back_c)
    back_xy = rs_xy(1)
    arrived(back_xy)
    back_z = rs_z(1)
    act_start(2)
    act_start(3)
    arrived(back_z)
    gated = rs_end(1) * gain_two
    mean = jnp.mean(x_two * gated, axis=1, keepdims=True)
    grad_mid = (
        gout_ref[...].astype(f32) + inv_two * gated - x_two * inv_two * inv_two * inv_two * mean
    ).astype(bf16)
    gm[r, z, x, core] = grad_mid
    gmid_ref[...] = grad_mid.astype(f32)
    cot_one_z = ag_z(gm, 3)
    arrived(cot_one_z)
    cot_one_xy = ag_xy(gm, 3)

    def out_slot(dr):
        return lambda k: own_out[pick[tiles + k], :, lanes_of(dr)]

    def mine(k):
        return pick[2 * tiles + k] > 0

    arrived(act_copies)
    last_c = rs_core(
        2,
        [act2] + [act2_far.at[dr - 1] for dr in range(1, rows)],
        [out_slot((rows - dr) % rows) for dr in range(rows)],
        mine,
    )
    arrived(cot_one_xy)
    cot_one_c = ag_core(gm, 3)
    for dr in range(1, rows):
        cp = pltpu.make_async_copy(
            act2_far.at[dr - 1], act_out.at[lax.rem(r + rows - dr, rows)], out_sem.at[5 + dr]
        )
        cp.start()
        outs.append(cp)
    arrived(last_c)
    last_xy = rs_xy(2)
    arrived(cot_one_c)

    def hidden_grad(j, carry):
        at = pl.ds(pl.multiple_of(j * step, step), step)
        value = dot(flat_of(gm, 0, width), weights[1, :, at]) * slope1[:, at]
        dh1[:, :, :, at] = value.astype(bf16).reshape(groups, 2, tok, step)
        return carry

    lax.fori_loop(0, unit_steps, hidden_grad, 0)
    first_c = rs_core(3, [dh1], [in_rows])

    def weight_grad(m, left, right):
        rhs = right[...].reshape(all_tok, units)

        def tile(j, carry):
            at = pl.ds(pl.multiple_of(j * step, step), step)
            lhs = left[:, :, :, :, :, at].reshape(all_tok, step)
            to = pl.ds(j * (step // per), step // per)
            grads[m, to] = dot_tn(lhs, rhs).astype(bf16).reshape(step // per, per, units)
            return carry

        lax.fori_loop(0, width_steps, tile, 0)
        cp = pltpu.make_async_copy(grads.at[m], gr_out.at[:, m], out_sem.at[4 + m])
        cp.start()
        outs.append(cp)

    arrived(last_xy)
    last_z = rs_z(2)
    arrived(first_c)
    first_xy = rs_xy(3)
    weight_grad(1, gm, act1)
    arrived(last_z)
    hid_out[...] = (x_two + rs_end(2)).astype(bf16)
    arrived(first_xy)
    first_z = rs_z(3)
    weight_grad(0, g1, dh1)
    arrived(first_z)
    gated = rs_end(3) * gain_one
    mean = jnp.mean(x_one * gated, axis=1, keepdims=True)
    gtok_out[...] = (
        gmid_ref[...] + inv_one * gated - x_one * inv_one * inv_one * inv_one * mean
    ).astype(bf16)

    for cp in outs:
        cp.wait()
    for cp in sent:
        cp.wait_send()
    a2a_part(0).wait_send()
    a2a_part(1).wait_send()


def middle_call(dims, pick, tokens, grad_out, gains, flat_in, flat_out, tile_in, tile_out):
    rows, zs, xs, tok, width, units, per, slot_cap, tiles = dims
    cols = zs * xs * 2
    total = rows * cols
    groups = rows * zs * xs
    all_tok = total * tok
    f32, bf16 = jnp.float32, jnp.bfloat16
    shape = jax.ShapeDtypeStruct
    vmem = pl.BlockSpec(memory_space=pltpu.VMEM)
    hbm = pl.BlockSpec(memory_space=pl.ANY)
    lane = (rows, zs, xs, 2, tok, width)
    others = rows * xs
    dma = pltpu.SemaphoreType.DMA
    buf = pltpu.VMEM
    return pl.pallas_call(
        functools.partial(middle_kernel, dims),
        in_specs=[pl.BlockSpec(memory_space=pltpu.SMEM), vmem, vmem, vmem, hbm, hbm, hbm, hbm],
        out_specs=[vmem, vmem] + [hbm] * 5,
        out_shape=[
            shape((tok, width), bf16),
            shape((tok, width), bf16),
            shape((total, 2, per, units), bf16),
            shape((rows, groups, 2, tok, units), bf16),
            shape((groups, 2, tok, units), bf16),
            shape(lane, bf16),
            shape(lane, bf16),
        ],
        scratch_shapes=[
            buf((2,) + flat_in.shape, bf16),
            buf((2, rows, cols, per, units), bf16),
            buf((2, width, units), bf16),
            buf((rows,) + tile_in.shape[1:3] + (units,), bf16),
            buf(tile_out.shape[1:], bf16),
            buf((rows - 1, all_tok, units), bf16),
            buf((rows - 1, all_tok, units), bf16),
            buf(lane, bf16),
            buf(lane, bf16),
            buf(lane, bf16),
            buf(lane, bf16),
            buf((groups, 2, tok, units), bf16),
            buf((all_tok, units), f32),
            buf((all_tok, units), f32),
            buf((groups, 2, tok, units), bf16),
            buf((rows - 1, groups, 2, tok, units), bf16),
            buf((groups, 2, tok, units), bf16),
            buf((groups, 2, tok, units), bf16),
            buf((2, total, per, units), bf16),
            buf((4, groups, tok, width), bf16),
            buf((4, groups, tok, width), f32),
            buf((4, groups, tok, width), bf16),
            buf((4, rows, zs, xs, tok, width), bf16),
            buf((4, others, zs, tok, width), bf16),
            buf((4, zs, tok, width), bf16),
            buf((4, zs, tok, width), bf16),
            buf((tok, width), f32),
            buf((tok, width), f32),
            dma((2,)),
            dma((2,)),
            dma((2,)),
            dma((2,)),
            dma((rows, 2 * slot_cap)),
            dma((rows, 2 * slot_cap)),
            dma((4, zs + others)),
            dma((4, zs + others)),
            dma((4, zs + others)),
            dma((4, zs + others)),
            dma((rows, 4)),
            dma((rows, 4)),
            dma((rows,)),
            dma((rows,)),
            dma((6 + rows,)),
        ],
        compiler_params=pltpu.CompilerParams(
            has_side_effects=True, vmem_limit_bytes=63 * 1024 * 1024
        ),
        cost_estimate=pl.CostEstimate(
            flops=24 * all_tok * width * units, bytes_accessed=24 * width * units, transcendentals=0
        ),
        name="middle",
    )(pick, tokens, grad_out, gains, flat_in, flat_out, tile_in, tile_out)


def flat_both_kernel(cols, split, g, w_in, w_out, mom, sec, o_in, o_out, o_mom, o_sec):
    rows, units = g.shape[0], g.shape[-1]
    rows_in = cols * 16
    part = rows_in // split
    p = lax.broadcasted_iota(jnp.int32, (part, rows_in), 0) + pl.program_id(1) * part
    q = lax.broadcasted_iota(jnp.int32, (part, rows_in), 1)
    swap = (lax.rem(p, cols) == q // 16) & (p // cols == lax.rem(q, 16))
    swap = jnp.where(swap, 1.0, 0.0).astype(jnp.bfloat16)
    for m, (w, o) in enumerate(((w_in, o_in), (w_out, o_out))):
        for rt in range(rows):
            at = slice(rt * units, (rt + 1) * units)
            got = g[rt, :, m].reshape(rows_in, units)
            grad = jnp.dot(swap, got, preferred_element_type=jnp.float32)
            new = adam_update(w[:, at], grad, mom[m, :, at], sec[m, :, at])
            o[:, at], o_mom[m, :, at], o_sec[m, :, at] = new


def flat_both(w_in, w_out, g, mom, sec, dims):
    rows, zs, xs, tok, width, units, per, slot_cap, tiles = dims
    cols = zs * xs * 2
    split = 2
    part = cols * 16 // split
    block = rows * units
    thin = pl.BlockSpec((part, block), lambda i, h: (i * split + h, 0))
    wide = pl.BlockSpec((2, part, block), lambda i, h: (0, i * split + h, 0))
    got = pl.BlockSpec((rows, cols, 2, 16, units), lambda i, h: (0, 0, 0, i, 0))
    shape = jax.ShapeDtypeStruct
    return pl.pallas_call(
        functools.partial(flat_both_kernel, cols, split),
        grid=(per // 16, split),
        in_specs=[got, thin, thin, wide, wide],
        out_specs=[thin, thin, wide, wide],
        out_shape=[
            shape(w_in.shape, w_in.dtype),
            shape(w_out.shape, w_out.dtype),
            shape(mom.shape, mom.dtype),
            shape(sec.shape, sec.dtype),
        ],
        cost_estimate=pl.CostEstimate(
            flops=30 * mom.size, bytes_accessed=22 * mom.size, transcendentals=2 * mom.size
        ),
        name="flat_both",
    )(g.reshape(rows, cols, 2, per, units), w_in, w_out, mom, sec)


def slot_kernel_part(m, tiles, live, left, right, w, mom, sec, *rest):
    o, o_mom, o_sec = rest[-3:]
    slot = pl.program_id(0)
    step = w.shape[-1]
    units = right.shape[-1]
    at = pl.program_id(1) * step
    row, lane = at // units, pl.multiple_of(lax.rem(at, units), step)
    grad = dot_tn(left[...], right[row, :, pl.ds(lane, step)])
    alive = live[m, slot] > 0
    old_w, old_m, old_s = w[0, 0], mom[0, 0, 0], sec[0, 0, 0]
    new_w, new_m, new_s = adam_update(old_w, grad, old_m, old_s)
    o[0, 0] = jnp.where(alive, new_w.astype(jnp.float32), old_w.astype(jnp.float32)).astype(
        jnp.bfloat16
    )
    o_mom[0, 0, 0] = jnp.where(alive, new_m, old_m)
    o_sec[0, 0, 0] = jnp.where(alive, new_s, old_s)


def slot_part(m, tiles, live, left, right, w, mom, sec, before=()):
    slot_cap, tile_rows, width = w.shape[1:]
    toks = left.shape[0]
    step = min(right.shape[-1], 1024)
    thin = pl.BlockSpec((1, 1, tile_rows, step), lambda s, h, *unused: (0, s, 0, h))
    wide = pl.BlockSpec((1, 1, 1, tile_rows, step), lambda s, h, *unused: (m, 0, s, 0, h))
    shape = jax.ShapeDtypeStruct
    return pl.pallas_call(
        functools.partial(slot_kernel_part, m),
        grid_spec=pltpu.PrefetchScalarGridSpec(
            num_scalar_prefetch=2,
            grid=(slot_cap, width // step),
            in_specs=[
                pl.BlockSpec((toks, tile_rows), lambda s, h, tiles, live: (0, tiles[m, s])),
                pl.BlockSpec(right.shape, lambda s, h, *unused: (0, 0, 0)),
                thin,
                wide,
                wide,
            ]
            + [pl.BlockSpec(memory_space=pl.ANY)] * len(before),
            out_specs=[thin, wide, wide],
        ),
        out_shape=[
            shape(w.shape, w.dtype),
            shape(mom.shape, mom.dtype),
            shape(sec.shape, sec.dtype),
        ],
        input_output_aliases={7 + i: 1 + i for i in range(len(before))},
        cost_estimate=pl.CostEstimate(
            flops=10**10, bytes_accessed=22 * w.size, transcendentals=2 * w.size
        ),
        name="slot_part",
    )(tiles, live, left, right, w, mom, sec, *before)


def fused_dims(row_total, col_total, tokens, flat_in, tile_in, owners):
    depth = 4 if col_total % 8 == 0 else 1
    across = col_total // (2 * depth)
    total = row_total * col_total
    tok, width = tokens.shape
    units = flat_in.shape[1] // row_total
    per = width // total
    slot_cap, tile_rows = tile_in.shape[1:3]
    tiles = owners.shape[-1]
    fits = (
        col_total % 2 == 0
        and width % total == 0
        and tok % 16 == 0
        and per % 16 == 0
        and units % 256 == 0
        and tile_rows == 256
        and tiles * tile_rows == width
        and total * tok * (width * 30 + units * 16) + width * units * 24 < 60 * 2**20
    )
    return (row_total, depth, across, tok, width, units, per, slot_cap, tiles) if fits else None


def fused_shards(
    dims,
    tokens,
    grad_out,
    gains,
    flat_in,
    flat_out,
    flat_moment,
    flat_second,
    tile_in,
    tile_out,
    tile_moment,
    tile_second,
    owners,
):
    rows, zs, xs, tok, width, units, per, slot_cap, tiles = dims
    cols = zs * xs * 2
    all_tok = rows * cols * tok
    row_index = lax.axis_index("row")
    owner_rows = owners[:, 0, :]
    ranks = tile_ranks(owner_rows)
    owned = (owner_rows == row_index).astype(jnp.int32)
    slot_of = owner_rows[0] * slot_cap + ranks[0]
    pick = jnp.concatenate([slot_of, ranks[1] * owned[1], owned[1]]).astype(jnp.int32)
    slot_ids = jnp.arange(slot_cap, dtype=jnp.int32)[None, :, None]
    mine = (owner_rows == row_index)[:, None, :] & (ranks[:, None, :] == slot_ids)
    positions = jnp.arange(tiles, dtype=jnp.int32)
    my_tiles = jnp.sum(jnp.where(mine, positions, 0), axis=-1).astype(jnp.int32)
    my_live = jnp.any(mine, axis=-1).astype(jnp.int32)

    hidden_out, grad_tokens, grads, act, d_hidden, normed, cot = middle_call(
        dims, pick, tokens, grad_out, gains, flat_in, flat_out, tile_in, tile_out
    )
    act_rows = act.reshape(rows, all_tok, units)
    d_hidden = d_hidden.reshape(all_tok, units)

    def by_row(value):
        got = [value]
        for shift in range(1, rows):
            pairs = [(src, (src + shift) % rows) for src in range(rows)]
            got.append(lax.ppermute(value, "row", pairs))
        ids = [lax.rem(row_index - shift + rows, rows) for shift in range(rows)]
        if rows == 2:
            first = row_index == 0
            return jnp.stack([jnp.where(first, got[0], got[1]), jnp.where(first, got[1], got[0])])
        placed = jnp.zeros((rows,) + value.shape, value.dtype)
        for where, piece in zip(ids, got):
            placed = lax.dynamic_update_index_in_dim(placed, piece, where, 0)
        return placed

    d_hidden_rows = by_row(d_hidden)

    def spread(grad):
        return lax.all_to_all(grad, both, split_axis=0, concat_axis=0, tiled=True)

    pair = spread(grads.reshape(rows * cols, 2 * per, units))
    tile_w_out, tile_m, tile_s = slot_part(
        1, my_tiles, my_live, cot.reshape(all_tok, width), act_rows, tile_out, tile_moment, tile_second
    )
    tile_w_in, tile_m, tile_s = slot_part(
        0,
        my_tiles,
        my_live,
        normed.reshape(all_tok, width),
        d_hidden_rows,
        tile_in,
        tile_moment,
        tile_second,
        (tile_m, tile_s),
    )
    new_in, new_out, moment, second = flat_both(
        flat_in, flat_out, pair, flat_moment, flat_second, dims
    )
    new_tile = (tile_w_in, tile_w_out, tile_m, tile_s)
    return (hidden_out, grad_tokens, new_in, new_out, moment, second, *new_tile)


def solution(mesh):
    return jax.shard_map(
        shards,
        mesh=mesh,
        in_specs=(
            P(("row", "col"), None),
            P(("row", "col"), None),
            P(),
            P(("row", "col"), None),
            P(("row", "col"), None),
            P(None, ("row", "col"), None),
            P(None, ("row", "col"), None),
            P("col", "row", None, None),
            P("col", "row", None, None),
            P(None, "col", "row", None, None),
            P(None, "col", "row", None, None),
            P(None, "col", None),
        ),
        out_specs=(
            P(("row", "col"), None),
            P(("row", "col"), None),
            P(("row", "col"), None),
            P(("row", "col"), None),
            P(None, ("row", "col"), None),
            P(None, ("row", "col"), None),
            P("col", "row", None, None),
            P("col", "row", None, None),
            P(None, "col", "row", None, None),
            P(None, "col", "row", None, None),
        ),
        check_vma=False,
    )
```
